32 devices in a mesh: dp: 8 (over y, x, core), fsdp: 4 (over z).
Axes of the slice: x: 2, y: 2, z: 4, core: 2. Of those that a mesh axis runs over, the one named last changes fastest.
Arguments:
- grads: float32 [32, 96, 128], P(('dp', 'fsdp')), may hold values from -0.6 to 0.6
- last_peak: float32 [96], replicated, may hold values from 0.05 to 0.8
- master: float32 [96, 128], P(('dp', 'fsdp')), may hold values from -6 to 6
- moment1: float32 [96, 128], P(('dp', 'fsdp')), may hold values from -6 to 6
- moment2: float32 [96, 128], P(('dp', 'fsdp')), may hold values from 0.25 to 8
Outputs:
- new_master: float32 [96, 128], P(('dp', 'fsdp'))
- new_moment1: float32 [96, 128], P(('dp', 'fsdp'))
- new_moment2: float32 [96, 128], P(('dp', 'fsdp'))
- weights: bfloat16 [96, 128], replicated
- block_peak: float32 [96], replicated
The draws below stay inside these ranges and needn't reach their ends.
All inputs are finite; a program needn't handle non-finite values.
Results may differ from the reference program's by a relative error of at most 0.0035.
Values may be sent and summed in bfloat16 or wider, within the bound.
A program may use at most 64 MiB of HBM per device.

```python
import math
import jax
import jax.numpy as jnp
from jax import lax

BLOCK = 128
STEP_COUNT = 10
REPLICAS = 32
BLOCKS = 96


def strengthened(values, stream_key, source, target, parts, factor):
    def block_of(dim):
        return (jnp.arange(values.shape[dim]) // (values.shape[dim] // parts)).reshape((-1,) + (1,) * (values.ndim - 1 - dim))

    first = jax.random.permutation(stream_key, parts)[block_of(target)]
    other_side = (block_of(target) + parts // 2) % parts
    return jnp.where((block_of(source) == first) | (block_of(source) == other_side), factor * values, values)


def level_of(key, extent, split, low, high):
    factor_of, own = 1.0, jax.random.fold_in(key, 6)
    for axis_at, shards_of in split:
        draws = jnp.exp(jax.random.uniform(jax.random.fold_in(own, axis_at), (shards_of,), jnp.float32, low / len(split), high / len(split)))
        factor_of = factor_of * jnp.repeat(draws, extent[axis_at] // shards_of).reshape([-1 if axis == axis_at else 1 for axis in range(len(extent))])
    return factor_of


def scatter_about(own_key, extent, spread, reach, shards=(), kind=jnp.bfloat16):
    drawn = spread * jax.random.normal(own_key, extent, jnp.float32)
    if shards:
        drawn = drawn * level_of(own_key, extent, shards, -0.22, 0.18)
    return jnp.clip(drawn, -reach, reach).astype(kind)


def gaussian_with(own_key, shape, width, most, cuts, heavy, held_as=jnp.bfloat16):
    entries = width * jax.random.normal(own_key, shape, jnp.float32)
    if cuts:
        entries = entries * level_of(own_key, shape, cuts, -0.22, 0.18)
    return jnp.clip(strengthened(entries, jax.random.fold_in(own_key, 3), *heavy), -most, most).astype(held_as)


def setup_inputs(seed: int = 0) -> dict:
    seeds = jax.random.split(jax.random.key(seed), 6)
    return {
        "grads": gaussian_with(seeds[0], (REPLICAS, BLOCKS, BLOCK), 0.1, 0.6, ((0, 32),), (0, 1, 32, 2.75), jnp.float32),
        "last_peak": jnp.clip(jnp.exp(jax.random.uniform(seeds[1], (BLOCKS,), jnp.float32, math.log(0.05), math.log(0.8))), 0.05, 0.8),
        "master": scatter_about(seeds[2], (BLOCKS, BLOCK), 1.0, 6.0, ((0, 32),), jnp.float32),
        "moment1": scatter_about(seeds[3], (BLOCKS, BLOCK), 1.0, 6.0, ((0, 32),), jnp.float32),
        "moment2": jnp.clip(jnp.exp(math.log(8.0) - 3.465736 * jax.random.uniform(seeds[4], (BLOCKS, BLOCK), jnp.float32) ** level_of(seeds[4], (BLOCKS, BLOCK), ((0, 32),), -0.2, 0.2)), 0.25, 8.0),
    }


code_limit = 448.0
peak_floor = 0.05
beta_one = 0.9
beta_two = 0.95
learn_rate = 0.05
decay_rate = 0.1
epsilon = 1e-08

def quantize(rows, inverse):
    codes = jnp.clip(rows * inverse[:, None], -code_limit, code_limit).astype(jnp.bfloat16)
    return lax.optimization_barrier(codes).astype(jnp.float32)

def adamw(gradient, master, moment1, moment2):
    first = beta_one * moment1 + (1.0 - beta_one) * gradient
    second = beta_two * moment2 + (1.0 - beta_two) * gradient * gradient
    corrected_one = first / (1.0 - beta_one ** STEP_COUNT)
    corrected_two = second / (1.0 - beta_two ** STEP_COUNT)
    updated = master - learn_rate * (corrected_one / (jnp.sqrt(corrected_two) + epsilon) + decay_rate * master)
    return (updated, first, second)

def reference(grads, last_peak, master, moment1, moment2):

    def peak_step(carry, slab):
        return (jnp.maximum(carry, lax.optimization_barrier(jnp.max(jnp.abs(slab), axis=1))), None)
    peak, unused = lax.scan(peak_step, jnp.zeros((grads.shape[1],), jnp.float32), grads)
    floored = jnp.maximum(last_peak, peak_floor)
    inverse = code_limit / floored
    scale = floored / code_limit

    def add_step(total, slab):
        return (total + quantize(slab, inverse), None)
    summed, unused = lax.scan(add_step, jnp.zeros(grads.shape[1:], jnp.float32), grads)
    gradient = summed * scale[:, None]
    updated, first, second = adamw(gradient, master, moment1, moment2)
    return (updated, first, second, updated.astype(jnp.bfloat16), peak)
```

```python
import functools

import jax
import jax.numpy as jnp
from jax import lax
from jax.experimental import pallas as pl
from jax.experimental.pallas import tpu as pltpu
from jax.sharding import PartitionSpec as P

STEP_COUNT = 10


code_limit = 448.0
peak_floor = 0.05
beta_one = 0.9
beta_two = 0.95
learn_rate = 0.05
decay_rate = 0.1
epsilon = 1e-08
AXES = ("dp", "fsdp")
UNROLL_MOST = 64
ROOT_BYTES = 8 * 2**20


def adamw(gradient, master, moment1, moment2):
    first = beta_one * moment1 + (1.0 - beta_one) * gradient
    second = beta_two * moment2 + (1.0 - beta_two) * gradient * gradient
    corrected_one = first * (1.0 / (1.0 - beta_one**STEP_COUNT))
    corrected_two = second * (1.0 / (1.0 - beta_two**STEP_COUNT))
    updated = master - learn_rate * (
        corrected_one / (jnp.sqrt(corrected_two) + epsilon) + decay_rate * master
    )
    return (updated, first, second)


def layout(sizes, blocks, width):
    dp, fsdp = sizes
    pair = 2 if dp % 2 == 0 else 1
    above = min(1, fsdp - 1)
    proxies = [(pair * q + pair - 1, above) for q in range(dp // pair)]
    collector = (min(3, dp - 1), 0)
    mates = [(k, 0) for k in range(pair)]
    fits = 2 * dp * fsdp * blocks * width <= ROOT_BYTES
    if above == 0 or pair == 1 or dp < 4 * pair or dp % (2 * pair) or not fits:
        mates = []
    return pair, proxies, collector, mates


def gathering(sizes):
    dp, fsdp = sizes
    half = dp // 4
    places = [(2 * g + 1 if g == half else 2 * (g - half) + 1, 0) for g in range(half, 2 * half)]
    return min(2, fsdp - 1), half, places


def kernel(
    sizes,
    grads_hbm,
    last_peak_hbm,
    master_hbm,
    moment1_hbm,
    moment2_hbm,
    updated_ref,
    first_ref,
    second_ref,
    weights_ref,
    peak_ref,
    grads,
    last_peak,
    state,
    codes,
    message,
    received,
    states,
    column,
    gradient_out,
    gradient_in,
    peak_message,
    peak_received,
    peak_out,
    peak_in,
    in_sems,
    recv_sems,
    send_sem,
    state_send,
    state_recv,
    grad_send,
    grad_recv,
    out_send,
    out_recv,
    peak_send,
    peak_recv,
    top_send,
    top_recv,
    *root_refs,
):
    dp, fsdp = sizes
    n = dp * fsdp
    blocks, width = message.shape
    pair, proxies, collector, mates = layout(sizes, blocks, width)
    count = len(proxies)
    hubs = proxies + [collector] + mates
    owned = blocks // n
    part = blocks // count
    lines = peak_out.shape[0]
    mine, level = lax.axis_index("dp"), lax.axis_index("fsdp")
    me = mine * fsdp + level
    slot = level * dp + mine
    group = lax.div(mine, pair)
    seat = lax.rem(mine, pair) * fsdp + level

    def at_place(where):
        return jnp.logical_and(mine == where[0], level == where[1])

    def any_of(flags):
        return functools.reduce(jnp.logical_or, flags, jnp.bool_(False))

    def unless(flag):
        return pl.when(jnp.logical_not(flag))

    is_proxy = any_of([at_place(where) for where in proxies])
    is_collector = at_place(collector)
    is_mate = any_of([at_place(where) for where in mates])
    is_hub = any_of([is_proxy, is_collector, is_mate])
    if mates:
        root = mates[-1]
        is_root = at_place(root)
        skip, kept = part, blocks - part
        rest = message.at[pl.ds(skip, kept)]
        is_kept = me * owned >= skip
        mate = mates[0]
        is_first = at_place(mate)
        near_levels, half, combiners = gathering(sizes)
        nears = []
        for at in range(half):
            chip = (half + at) * pair
            nears.append([(k, f) for f in range(near_levels) for k in range(chip, chip + pair)])
        in_nears = [jnp.logical_and(level < near_levels, group == half + at) for at in range(half)]
        is_near = any_of(in_nears)
        idle = [where for where, near in zip(combiners, nears) if where in near]
        is_idle = any_of([at_place(where) for where in idle])
        (
            all_received,
            all_states,
            all_column,
            near_received,
            partial_out,
            partial_in,
            all_recv,
            all_send,
            all_state_send,
            all_state_recv,
            near_recv,
            partial_send,
            partial_recv,
            early_out,
            early_in,
            early_send,
            early_recv,
            far_send,
            mate_state_send,
        ) = root_refs

    def remote(source, target, send, recv, where):
        return pltpu.make_async_remote_copy(
            src_ref=source,
            dst_ref=target,
            send_sem=send,
            recv_sem=recv,
            device_id=where,
            device_id_type=pl.DeviceIdType.MESH,
        )

    def drain(ref, sem):
        pltpu.make_async_copy(ref, ref, sem).wait()

    def others(step, skipped=()):
        if n <= UNROLL_MOST:
            near = [(k, f) for f in range(fsdp) for k in range(pair)]
            far = [(k, f) for f in range(fsdp) for k in range(pair, dp)]
            for where in near + far:
                if where not in skipped:
                    unless(at_place(where))(functools.partial(step, where))
        else:

            def turn(k, carry):
                other = lax.rem(me + k, n)
                step((lax.div(other, fsdp), lax.rem(other, fsdp)))
                return carry

            lax.fori_loop(1, n, turn, 0)

    loads = [
        pltpu.make_async_copy(source, target, in_sems.at[at])
        for at, (source, target) in enumerate(
            (
                (last_peak_hbm, last_peak),
                (grads_hbm.at[:, pl.ds(0, part)], grads.at[:, pl.ds(0, part)]),
                (grads_hbm.at[:, pl.ds(part, blocks - part)], grads.at[:, pl.ds(part, blocks - part)]),
                (master_hbm, state.at[0]),
                (moment1_hbm, state.at[1]),
                (moment2_hbm, state.at[2]),
            )
        )
    ]
    for load in loads:
        load.start()
    barrier = pltpu.get_barrier_semaphore()

    def greet(where):
        pl.semaphore_signal(
            barrier, inc=1, device_id=where, device_id_type=pl.DeviceIdType.MESH
        )

    @pl.when(is_hub)
    def _():
        others(greet)

    if mates:

        for combiner, near in zip(combiners, nears):
            if combiner not in hubs:

                @pl.when(at_place(combiner))
                def _():
                    for where in near:
                        if where != combiner:
                            greet(where)

    loads[0].wait()
    floored = jnp.maximum(last_peak[...], peak_floor)
    inverse = code_limit / floored
    scale = floored / code_limit
    row = lax.broadcasted_iota(jnp.int32, (blocks, blocks), 0)
    lane = lax.broadcasted_iota(jnp.int32, (blocks, blocks), 1)
    diagonal = row == lane
    inverse_column = jnp.sum(jnp.where(diagonal, inverse, 0.0), axis=1, keepdims=True)
    def encode(first, rows):
        scaled = grads[0, pl.ds(first, rows), :] * inverse_column[first : first + rows]
        message[pl.ds(first, rows), :] = jnp.clip(scaled, -code_limit, code_limit).astype(jnp.bfloat16)

    loads[1].wait()
    encode(0, part)

    if mates:
        greeted_more = any_of(
            [flag for flag, combiner in zip(in_nears, combiners) if combiner not in hubs]
        )
        greeted_more = jnp.logical_and(greeted_more, jnp.logical_not(is_idle))
        for flag, more in ((greeted_more, 1), (jnp.logical_not(greeted_more), 0)):

            @pl.when(jnp.logical_and(flag, is_hub))
            def _():
                pl.semaphore_wait(barrier, len(hubs) - 1 + more)

            @pl.when(jnp.logical_and(flag, jnp.logical_not(is_hub)))
            def _():
                pl.semaphore_wait(barrier, len(hubs) + more)

    else:

        @pl.when(is_hub)
        def _():
            pl.semaphore_wait(barrier, len(hubs) - 1)

        @unless(is_hub)
        def _():
            pl.semaphore_wait(barrier, len(hubs))

    last = fsdp - 1
    lateness = lax.div(level, max(last, 1))

    def send_part(q, where):
        @unless(at_place(where))
        def _():
            source = message.at[pl.ds(q * part, part)]
            remote(source, received.at[slot], send_sem, recv_sems.at[level], where).start()

    if mates:

        @pl.when(level == last)
        def _():
            source = message.at[pl.ds(0, part)]
            remote(source, received.at[slot], far_send, recv_sems.at[level], mate).start()

        @unless(level == last)
        def _():
            send_part(0, proxies[0])

    else:
        send_part(0, proxies[0])
    loads[2].wait()
    encode(part, blocks - part)
    values = grads[0]

    if mates:

        @unless(jnp.logical_or(is_root, is_near))
        def _():
            remote(rest, all_received.at[slot], all_send, all_recv.at[level], root).start()

        for at, combiner in enumerate(combiners):

            @pl.when(jnp.logical_and(in_nears[at], jnp.logical_not(at_place(combiner))))
            def _():
                target = near_received.at[level * pair + mine - (half + at) * pair]
                remote(rest, target, all_send, near_recv, combiner).start()

        @pl.when(level == last)
        def _():
            send_part(0, proxies[0])

    for load in loads[3:]:
        load.wait()
    if mates:

        @pl.when(is_kept)
        def _():
            target = all_states.at[me - skip // owned]
            remote(state, target, all_state_send, all_state_recv.at[lateness], root).start()

        @pl.when(jnp.logical_and(group == 0, jnp.logical_not(is_first)))
        def _():
            target = states.at[seat]
            remote(state, target, mate_state_send, state_recv.at[lateness], mate).start()

    for q, where in enumerate(proxies):

        @pl.when(jnp.logical_and(group == q, jnp.logical_not(is_proxy)))
        def _():
            remote(state, states.at[seat], state_send, state_recv.at[lateness], where).start()

    peak_column = jnp.max(jnp.abs(values), axis=1, keepdims=True)
    peak_row = jnp.max(jnp.where(diagonal, peak_column, 0.0), axis=0, keepdims=True)
    peak_message[...] = jnp.zeros_like(peak_message)
    for line in range(lines):
        low = line * width
        high = min(low + width, blocks)
        peak_message[pl.ds(line, 1), : high - low] = peak_row[:, low:high]

    for where in mates + [collector]:

        @unless(at_place(where))
        def _():
            remote(peak_message, peak_received.at[me], peak_send, peak_recv, where).start()

    for q, where in list(enumerate(proxies))[1:]:
        send_part(q, where)

    def top_of_all():
        peak_received[me] = peak_message[...]
        drain(peak_received.at[pl.ds(0, n - 1)], peak_recv)
        return jnp.max(peak_received[...], axis=0)

    def column_of(values, first, rows):
        at_row = lax.broadcasted_iota(jnp.int32, (rows, blocks), 0)
        at_lane = lax.broadcasted_iota(jnp.int32, (rows, blocks), 1)
        return jnp.sum(jnp.where(at_lane == at_row + first, values, 0.0), axis=1, keepdims=True)

    def run_if(flag, step):
        if isinstance(flag, bool):
            if flag:
                step()
        else:
            pl.when(flag)(step)

    def negated(flag):
        return not flag if isinstance(flag, bool) else jnp.logical_not(flag)

    def place_states(target, source, owners, late):
        for at in range(owners):
            if (at % fsdp == last) == late:
                for kind in range(3):
                    target[kind, pl.ds(at * owned, owned), :] = source[at, kind]

    def summed(inbox, first, rows):
        return jnp.sum(inbox[pl.ds(first, rows)].astype(jnp.float32), axis=0)

    if mates:
        for at, (combiner, near) in enumerate(zip(combiners, nears)):

            @pl.when(at_place(combiner))
            def _():
                own = combiner in near
                if own:
                    near_received[near.index(combiner)] = message[pl.ds(skip, kept), :]
                drain(near_received.at[pl.ds(0, len(near) - own)], near_recv)
                partial_out[...] = summed(near_received, 0, len(near))
                remote(partial_out, partial_in.at[at], partial_send, partial_recv, root).start()

    @pl.when(is_collector)
    def _():
        top = top_of_all()
        peak_out[...] = top

        def spread_top(where):
            remote(peak_out, peak_in, top_send, top_recv, where).start()

        others(spread_top, mates)
        peak_in[...] = top

    if mates:

        @pl.when(is_root)
        def _():
            all_received[slot] = message[pl.ds(skip, kept), :]
            own_scale = column_of(scale, skip, kept)
            owners = kept // owned
            total = None
            for f in range(fsdp):
                direct = dp // 2 if f < near_levels else dp
                if f == last:
                    drain(all_states.at[pl.ds(0, (dp - pair) * last)], all_state_recv.at[0])
                    place_states(all_column, all_states, owners, False)
                    drain(partial_in, partial_recv)
                    total = total + summed(partial_in, 0, half)
                    drain(all_states.at[pl.ds(0, dp - pair)], all_state_recv.at[1])
                    place_states(all_column, all_states, owners, True)
                drain(all_received.at[pl.ds(0, direct - (f == root[1]))], all_recv.at[f])
                more = summed(all_received, f * dp, direct)
                total = more if total is None else total + more
            gradient = total * own_scale
            updated, _, _ = adamw(gradient, all_column[0], all_column[1], all_column[2])
            ready = weights_ref.at[pl.ds(skip, kept)]
            weights_ref[pl.ds(skip, kept), :] = updated.astype(jnp.bfloat16)
            for where in mates[:-1]:
                remote(ready, ready, out_send, out_recv, where).start()

    if mates:

        @pl.when(is_first)
        def _():
            states[pl.ds(seat, 1)] = state[...][None]
            own_scale = column_of(scale, 0, part)
            drain(states.at[pl.ds(0, pair * last - 1)], state_recv.at[0])
            place_states(column, states, pair * fsdp, False)
            drain(states.at[pl.ds(0, pair)], state_recv.at[1])
            place_states(column, states, pair * fsdp, True)
            drain(early_in, early_recv)
            drain(received.at[pl.ds(0, dp)], recv_sems.at[last])
            gradient = (early_in[...] + summed(received, last * dp, dp)) * own_scale
            codes[...] = gradient
            own = (mate[0] * fsdp + mate[1]) * owned
            gradient_in[...] = codes[pl.ds(own, owned), :]
            updated, _, _ = adamw(gradient, column[0], column[1], column[2])
            weights_ref[pl.ds(0, part), :] = updated.astype(jnp.bfloat16)

    def reduce_part(mine, level):
        group = mine // pair if isinstance(mine, int) else lax.div(mine, pair)
        seat = (mine - group * pair) * fsdp + level
        first = group * part
        if not isinstance(first, int):
            first = pl.multiple_of(first, 8)
        received[pl.ds(level * dp + mine, 1)] = message[pl.ds(first, part)][None]
        states[pl.ds(seat, 1)] = state[...][None]
        own_scale = column_of(scale, first, part)
        at_last = proxies[0][1] == last
        total = None
        for f in range(fsdp):
            if f == last:
                if mates and group == 0:
                    early_out[...] = total
                    remote(early_out, early_in, early_send, early_recv, mate).start()
                drain(states.at[pl.ds(0, pair * last - (not at_last))], state_recv.at[0])
                place_states(column, states, pair * fsdp, False)
                drain(states.at[pl.ds(0, pair - at_last)], state_recv.at[1])
                place_states(column, states, pair * fsdp, True)
            own_level = level == f
            run_if(own_level, lambda: drain(received.at[pl.ds(0, dp - 1)], recv_sems.at[f]))
            run_if(negated(own_level), lambda: drain(received.at[pl.ds(0, dp)], recv_sems.at[f]))
            more = summed(received, f * dp, dp)
            total = more if total is None else total + more
        gradient = total * own_scale
        codes[...] = gradient

        def hand_out(at):
            gradient_out[at] = codes[pl.ds(at * owned, owned), :]
            where = (group * pair + at // fsdp, at % fsdp)

            def send():
                remote(gradient_out.at[at], gradient_in, grad_send, grad_recv, where).start()

            run_if(negated(seat == at), send)

        lines_of = pl.ds(first, part)
        ready = weights_ref.at[lines_of]

        def spread(where):
            remote(ready, ready, out_send, out_recv, where).start()

        served = [root] if mates and group == 0 else []
        early = [where[0] * fsdp + where[1] for where in served]
        skipped = [mate[0] * fsdp + mate[1]] if served else []
        late = [at for at in range(pair * fsdp) if at not in early + skipped]
        for at in early if served else late:
            hand_out(at)
        updated, _, _ = adamw(gradient, column[0], column[1], column[2])
        weights_ref[lines_of, :] = updated.astype(jnp.bfloat16)
        for where in served:
            spread(where)
        for at in late if served else early:
            hand_out(at)
        if isinstance(mine, int):
            for where in [(k, f) for k in range(dp) for f in range(fsdp)]:
                if where != (mine, level) and where not in mates:
                    spread(where)
        else:
            others(spread)
        gradient_in[...] = gradient_out[seat]

    if mates:
        for where in proxies:
            pl.when(at_place(where))(functools.partial(reduce_part, *where))
    else:
        pl.when(is_proxy)(functools.partial(reduce_part, mine, level))

    @unless(jnp.logical_or(is_proxy, is_first) if mates else is_proxy)
    def _():
        drain(gradient_in, grad_recv)

    updated, first, second = adamw(gradient_in[...], state[0], state[1], state[2])
    updated_ref[...] = updated
    first_ref[...] = first
    second_ref[...] = second

    @pl.when(is_mate)
    def _():
        peak_in[...] = top_of_all()

    @unless(any_of([is_collector, is_mate]))
    def _():
        drain(peak_in, top_recv)

    for line in range(lines):
        low = line * width
        high = min(low + width, blocks)
        peak_ref[:, low:high] = peak_in[pl.ds(line, 1), : high - low]

    @unless(is_proxy)
    def _():
        drain(message, send_sem)
        drain(state, state_send)

    @pl.when(is_proxy)
    def _():
        drain(message.at[pl.ds(0, (count - 1) * part)], send_sem)

    if mates:

        @unless(jnp.logical_or(is_root, is_idle))
        def _():
            drain(rest, all_send)

        @pl.when(is_kept)
        def _():
            drain(state, all_state_send)

        @pl.when(any_of([at_place(where) for where in combiners]))
        def _():
            drain(partial_out, partial_send)

        @pl.when(at_place(proxies[0]))
        def _():
            drain(early_out, early_send)

        @pl.when(level == last)
        def _():
            drain(message.at[pl.ds(0, part)], far_send)

        @pl.when(jnp.logical_and(group == 0, jnp.logical_not(is_first)))
        def _():
            drain(state, mate_state_send)

    inboxes = len(mates) + 1
    is_inbox = any_of([is_mate, is_collector])

    @pl.when(is_inbox)
    def _():
        if inboxes > 1:
            drain(peak_received.at[pl.ds(0, inboxes - 1)], peak_send)

    @unless(is_inbox)
    def _():
        drain(peak_received.at[pl.ds(0, inboxes)], peak_send)

    @pl.when(is_proxy)
    def _():
        drain(weights_ref.at[pl.ds(0, (count - 1) * part)], out_recv)

    for at, where in enumerate(proxies):

        @pl.when(at_place(where))
        def _():
            unserved = 1 if mates and at == 0 else 0
            drain(gradient_out.at[pl.ds(0, pair * fsdp - 1 - unserved)], grad_send)

    if mates:

        @pl.when(is_root)
        def _():
            drain(weights_ref.at[pl.ds(0, skip)], out_recv)
            for where in mates[:-1]:
                drain(rest, out_send)

        @pl.when(is_first)
        def _():
            drain(rest, out_recv)

        @unless(any_of([is_proxy, is_mate]))
        def _():
            drain(weights_ref, out_recv)

        for at, where in enumerate(proxies):
            reached = n - 1 - (len(mates) if at else 1)

            @pl.when(at_place(where))
            def _():
                drain(received.at[pl.ds(0, reached)], out_send)

    else:

        @unless(is_proxy)
        def _():
            drain(weights_ref, out_recv)

        @pl.when(is_proxy)
        def _():
            drain(received.at[pl.ds(0, n - 1)], out_send)

    @pl.when(is_collector)
    def _():
        drain(peak_received.at[pl.ds(0, n - 1 - len(mates))], top_send)


def finish_kernel(*refs):
    count = (len(refs) - 1) // 2
    sems = refs[-1]
    stores = [
        pltpu.make_async_copy(refs[at], refs[count + at], sems.at[at])
        for at in range(count)
    ]
    for store in stores:
        store.start()
    for store in stores:
        store.wait()


def body(sizes, grads, last_peak, master, moment1, moment2):
    dp, fsdp = sizes
    n = dp * fsdp
    blocks, width = grads.shape[1:]
    pair, proxies, _, mates = layout(sizes, blocks, width)
    count = len(proxies)
    owned = master.shape[0]
    part = blocks // count
    lines = pl.cdiv(blocks, width)
    f32, bf16 = jnp.float32, jnp.bfloat16
    vmem = pl.BlockSpec(memory_space=pltpu.VMEM)
    anywhere = pl.BlockSpec(memory_space=pl.ANY)
    shapes = (
        ((owned, width), f32),
        ((owned, width), f32),
        ((owned, width), f32),
        ((blocks, width), bf16),
        ((1, blocks), f32),
    )
    kept = blocks - part
    near_levels, half, _ = gathering(sizes)
    root_scratch = [
        pltpu.VMEM((n, kept, width), bf16),
        pltpu.VMEM((kept // owned, 3, owned, width), f32),
        pltpu.VMEM((3, kept, width), f32),
        pltpu.VMEM((near_levels * pair, kept, width), bf16),
        pltpu.VMEM((kept, width), f32),
        pltpu.VMEM((half, kept, width), f32),
        pltpu.SemaphoreType.DMA((fsdp,)),
        pltpu.SemaphoreType.DMA,
        pltpu.SemaphoreType.DMA,
        pltpu.SemaphoreType.DMA((2,)),
        pltpu.SemaphoreType.DMA,
        pltpu.SemaphoreType.DMA,
        pltpu.SemaphoreType.DMA,
        pltpu.VMEM((part, width), f32),
        pltpu.VMEM((part, width), f32),
    ] + [pltpu.SemaphoreType.DMA] * 4
    results = pl.pallas_call(
        functools.partial(kernel, sizes),
        out_shape=tuple(pltpu.VMEM(shape, kind) for shape, kind in shapes),
        in_specs=[anywhere] * 5,
        out_specs=(vmem,) * 5,
        scratch_shapes=[
            pltpu.VMEM((1, blocks, width), f32),
            pltpu.VMEM((1, blocks), f32),
            pltpu.VMEM((3, owned, width), f32),
            pltpu.VMEM((part, width), f32),
            pltpu.VMEM((blocks, width), bf16),
            pltpu.VMEM((n, part, width), bf16),
            pltpu.VMEM((pair * fsdp, 3, owned, width), f32),
            pltpu.VMEM((3, part, width), f32),
            pltpu.VMEM((pair * fsdp, owned, width), f32),
            pltpu.VMEM((owned, width), f32),
            pltpu.VMEM((lines, width), f32),
            pltpu.VMEM((n, lines, width), f32),
            pltpu.VMEM((lines, width), f32),
            pltpu.VMEM((lines, width), f32),
            pltpu.SemaphoreType.DMA((6,)),
            pltpu.SemaphoreType.DMA((fsdp,)),
        ]
        + [pltpu.SemaphoreType.DMA] * 2
        + [pltpu.SemaphoreType.DMA((2,))]
        + [pltpu.SemaphoreType.DMA] * 8
        + (root_scratch if mates else []),
        compiler_params=pltpu.CompilerParams(collective_id=0, has_side_effects=True),
    )(grads, last_peak.reshape(1, blocks), master, moment1, moment2)
    updated, first, second, weights, peak = pl.pallas_call(
        finish_kernel,
        out_shape=tuple(jax.ShapeDtypeStruct(shape, kind) for shape, kind in shapes),
        in_specs=[vmem] * 5,
        out_specs=(anywhere,) * 5,
        scratch_shapes=[pltpu.SemaphoreType.DMA((5,))],
    )(*(pltpu.with_memory_space_constraint(result, pltpu.VMEM) for result in results))
    return (updated, first, second, weights, peak.reshape(blocks))


def solution(mesh):
    sharded = P(AXES, None)
    return jax.shard_map(
        functools.partial(body, (mesh.shape["dp"], mesh.shape["fsdp"])),
        mesh=mesh,
        in_specs=(P(AXES, None, None), P(), sharded, sharded, sharded),
        out_specs=(sharded, sharded, sharded, P(), P()),
        check_vma=False,
    )
```

```python
import functools

import jax
import jax.numpy as jnp
from jax import lax
from jax.experimental import pallas as pl
from jax.experimental.pallas import tpu as pltpu
from jax.sharding import PartitionSpec as P

STEP_COUNT = 10


code_limit = 448.0
peak_floor = 0.05
beta_one = 0.9
beta_two = 0.95
learn_rate = 0.05
decay_rate = 0.1
epsilon = 1e-08
AXES = ("dp", "fsdp")
UNROLL_MOST = 64
ROOT_BYTES = 8 * 2**20


def adamw(gradient, master, moment1, moment2):
    first = beta_one * moment1 + (1.0 - beta_one) * gradient
    second = beta_two * moment2 + (1.0 - beta_two) * gradient * gradient
    corrected_one = first * (1.0 / (1.0 - beta_one**STEP_COUNT))
    corrected_two = second * (1.0 / (1.0 - beta_two**STEP_COUNT))
    updated = master - learn_rate * (
        corrected_one / (jnp.sqrt(corrected_two) + epsilon) + decay_rate * master
    )
    return (updated, first, second)


def layout(sizes, blocks, width):
    dp, fsdp = sizes
    pair = 2 if dp % 2 == 0 else 1
    above = min(1, fsdp - 1)
    proxies = [(pair * q + pair - 1, above) for q in range(dp // pair)]
    collector = (min(3, dp - 1), 0)
    mates = [(k, 0) for k in range(pair)]
    fits = 2 * dp * fsdp * blocks * width <= ROOT_BYTES
    if above == 0 or pair == 1 or dp < 4 * pair or dp % (2 * pair) or not fits:
        mates = []
    return pair, proxies, collector, mates


def gathering(sizes):
    dp, fsdp = sizes
    chips = dp // 2
    count = chips // 4
    return min(2, fsdp - 1), count, [(2 * (g - chips // 2) + 1, 0) for g in range(chips - count, chips)]


def kernel(
    sizes,
    grads_hbm,
    last_peak_hbm,
    master_hbm,
    moment1_hbm,
    moment2_hbm,
    updated_ref,
    first_ref,
    second_ref,
    weights_ref,
    peak_ref,
    grads,
    last_peak,
    state,
    codes,
    message,
    received,
    states,
    column,
    gradient_out,
    gradient_in,
    peak_message,
    peak_received,
    peak_out,
    peak_in,
    in_sems,
    recv_sems,
    send_sem,
    state_send,
    state_recv,
    grad_send,
    grad_recv,
    out_send,
    out_recv,
    peak_send,
    peak_recv,
    top_send,
    top_recv,
    *root_refs,
):
    dp, fsdp = sizes
    n = dp * fsdp
    blocks, width = message.shape
    pair, proxies, collector, mates = layout(sizes, blocks, width)
    count = len(proxies)
    hubs = proxies + [collector] + mates
    owned = blocks // n
    part = blocks // count
    lines = peak_out.shape[0]
    mine, level = lax.axis_index("dp"), lax.axis_index("fsdp")
    me = mine * fsdp + level
    slot = level * dp + mine
    group = lax.div(mine, pair)
    seat = lax.rem(mine, pair) * fsdp + level

    def at_place(where):
        return jnp.logical_and(mine == where[0], level == where[1])

    def any_of(flags):
        return functools.reduce(jnp.logical_or, flags, jnp.bool_(False))

    def unless(flag):
        return pl.when(jnp.logical_not(flag))

    is_proxy = any_of([at_place(where) for where in proxies])
    is_collector = at_place(collector)
    is_mate = any_of([at_place(where) for where in mates])
    is_hub = any_of([is_proxy, is_collector, is_mate])
    if mates:
        root = mates[-1]
        is_root = at_place(root)
        skip, kept = part, blocks - part
        rest = message.at[pl.ds(skip, kept)]
        is_kept = me * owned >= skip
        mate = mates[0]
        is_first = at_place(mate)
        near_levels, gathered, combiners = gathering(sizes)
        tops = dp // pair - gathered
        nears = []
        for at in range(gathered):
            chip = (tops + at) * pair
            nears.append([(k, f) for f in range(near_levels) for k in range(chip, chip + pair)])
        in_nears = [jnp.logical_and(level < near_levels, group == tops + at) for at in range(gathered)]
        is_near = any_of(in_nears)
        idle = [where for where, near in zip(combiners, nears) if where in near]
        is_idle = any_of([at_place(where) for where in idle])
        (
            all_received,
            all_states,
            all_column,
            near_received,
            partial_out,
            partial_in,
            all_recv,
            all_send,
            all_state_send,
            all_state_recv,
            near_recv,
            partial_send,
            partial_recv,
            early_out,
            early_in,
            early_send,
            early_recv,
            far_send,
            mate_state_send,
        ) = root_refs

    def remote(source, target, send, recv, where):
        return pltpu.make_async_remote_copy(
            src_ref=source,
            dst_ref=target,
            send_sem=send,
            recv_sem=recv,
            device_id=where,
            device_id_type=pl.DeviceIdType.MESH,
        )

    def drain(ref, sem):
        pltpu.make_async_copy(ref, ref, sem).wait()

    def others(step, skipped=()):
        if n <= UNROLL_MOST:
            near = [(k, f) for f in range(fsdp) for k in range(pair)]
            far = [(k, f) for f in range(fsdp) for k in range(pair, dp)]
            for where in near + far:
                if where not in skipped:
                    unless(at_place(where))(functools.partial(step, where))
        else:

            def turn(k, carry):
                other = lax.rem(me + k, n)
                step((lax.div(other, fsdp), lax.rem(other, fsdp)))
                return carry

            lax.fori_loop(1, n, turn, 0)

    loads = [
        pltpu.make_async_copy(source, target, in_sems.at[at])
        for at, (source, target) in enumerate(
            (
                (last_peak_hbm, last_peak),
                (grads_hbm.at[:, pl.ds(0, part)], grads.at[:, pl.ds(0, part)]),
                (grads_hbm.at[:, pl.ds(part, blocks - part)], grads.at[:, pl.ds(part, blocks - part)]),
                (master_hbm, state.at[0]),
                (moment1_hbm, state.at[1]),
                (moment2_hbm, state.at[2]),
            )
        )
    ]
    for load in loads:
        load.start()
    barrier = pltpu.get_barrier_semaphore()

    def greet(where):
        pl.semaphore_signal(
            barrier, inc=1, device_id=where, device_id_type=pl.DeviceIdType.MESH
        )

    @pl.when(is_hub)
    def _():
        others(greet)

    if mates:

        for combiner, near in zip(combiners, nears):
            if combiner not in hubs:

                @pl.when(at_place(combiner))
                def _():
                    for where in near:
                        if where != combiner:
                            greet(where)

    loads[0].wait()
    floored = jnp.maximum(last_peak[...], peak_floor)
    inverse = code_limit / floored
    scale = floored / code_limit
    row = lax.broadcasted_iota(jnp.int32, (blocks, blocks), 0)
    lane = lax.broadcasted_iota(jnp.int32, (blocks, blocks), 1)
    diagonal = row == lane
    inverse_column = jnp.sum(jnp.where(diagonal, inverse, 0.0), axis=1, keepdims=True)
    def encode(first, rows):
        scaled = grads[0, pl.ds(first, rows), :] * inverse_column[first : first + rows]
        message[pl.ds(first, rows), :] = jnp.clip(scaled, -code_limit, code_limit).astype(jnp.bfloat16)

    loads[1].wait()
    encode(0, part)

    if mates:
        greeted_more = any_of(
            [flag for flag, combiner in zip(in_nears, combiners) if combiner not in hubs]
        )
        greeted_more = jnp.logical_and(greeted_more, jnp.logical_not(is_idle))
        for flag, more in ((greeted_more, 1), (jnp.logical_not(greeted_more), 0)):

            @pl.when(jnp.logical_and(flag, is_hub))
            def _():
                pl.semaphore_wait(barrier, len(hubs) - 1 + more)

            @pl.when(jnp.logical_and(flag, jnp.logical_not(is_hub)))
            def _():
                pl.semaphore_wait(barrier, len(hubs) + more)

    else:

        @pl.when(is_hub)
        def _():
            pl.semaphore_wait(barrier, len(hubs) - 1)

        @unless(is_hub)
        def _():
            pl.semaphore_wait(barrier, len(hubs))

    last = fsdp - 1
    lateness = lax.div(level, max(last, 1))

    def send_part(q, where):
        @unless(at_place(where))
        def _():
            source = message.at[pl.ds(q * part, part)]
            remote(source, received.at[slot], send_sem, recv_sems.at[level], where).start()

    if mates:

        @pl.when(level == last)
        def _():
            source = message.at[pl.ds(0, part)]
            remote(source, received.at[slot], far_send, recv_sems.at[level], mate).start()

        @unless(level == last)
        def _():
            send_part(0, proxies[0])

    else:
        send_part(0, proxies[0])
    loads[2].wait()
    encode(part, blocks - part)
    values = grads[0]

    if mates:

        @pl.when(level == last)
        def _():
            send_part(0, proxies[0])

        @unless(jnp.logical_or(is_root, is_near))
        def _():
            remote(rest, all_received.at[slot], all_send, all_recv.at[level], root).start()

        for at, combiner in enumerate(combiners):

            @pl.when(jnp.logical_and(in_nears[at], jnp.logical_not(at_place(combiner))))
            def _():
                target = near_received.at[level * pair + mine - (tops + at) * pair]
                remote(rest, target, all_send, near_recv, combiner).start()

    for load in loads[3:]:
        load.wait()
    if mates:

        @pl.when(is_kept)
        def _():
            target = all_states.at[me - skip // owned]
            remote(state, target, all_state_send, all_state_recv.at[lateness], root).start()

        @pl.when(jnp.logical_and(group == 0, jnp.logical_not(is_first)))
        def _():
            target = states.at[seat]
            remote(state, target, mate_state_send, state_recv.at[lateness], mate).start()

    for q, where in enumerate(proxies):

        @pl.when(jnp.logical_and(group == q, jnp.logical_not(is_proxy)))
        def _():
            remote(state, states.at[seat], state_send, state_recv.at[lateness], where).start()

    peak_column = jnp.max(jnp.abs(values), axis=1, keepdims=True)
    peak_row = jnp.max(jnp.where(diagonal, peak_column, 0.0), axis=0, keepdims=True)
    peak_message[...] = jnp.zeros_like(peak_message)
    for line in range(lines):
        low = line * width
        high = min(low + width, blocks)
        peak_message[pl.ds(line, 1), : high - low] = peak_row[:, low:high]

    for where in mates + [collector]:

        @unless(at_place(where))
        def _():
            remote(peak_message, peak_received.at[me], peak_send, peak_recv, where).start()

    for q, where in list(enumerate(proxies))[1:]:
        send_part(q, where)

    def top_of_all():
        peak_received[me] = peak_message[...]
        drain(peak_received.at[pl.ds(0, n - 1)], peak_recv)
        return jnp.max(peak_received[...], axis=0)

    def column_of(values, first, rows):
        at_row = lax.broadcasted_iota(jnp.int32, (rows, blocks), 0)
        at_lane = lax.broadcasted_iota(jnp.int32, (rows, blocks), 1)
        return jnp.sum(jnp.where(at_lane == at_row + first, values, 0.0), axis=1, keepdims=True)

    def run_if(flag, step):
        if isinstance(flag, bool):
            if flag:
                step()
        else:
            pl.when(flag)(step)

    def negated(flag):
        return not flag if isinstance(flag, bool) else jnp.logical_not(flag)

    def place_states(target, source, owners, late):
        for at in range(owners):
            if (at % fsdp == last) == late:
                for kind in range(3):
                    target[kind, pl.ds(at * owned, owned), :] = source[at, kind]

    def summed(inbox, first, rows):
        return jnp.sum(inbox[pl.ds(first, rows)].astype(jnp.float32), axis=0)

    if mates:
        for at, (combiner, near) in enumerate(zip(combiners, nears)):

            @pl.when(at_place(combiner))
            def _():
                own = combiner in near
                if own:
                    near_received[near.index(combiner)] = message[pl.ds(skip, kept), :]
                drain(near_received.at[pl.ds(0, len(near) - own)], near_recv)
                partial_out[...] = summed(near_received, 0, len(near))
                remote(partial_out, partial_in.at[at], partial_send, partial_recv, root).start()

    @pl.when(is_collector)
    def _():
        top = top_of_all()
        peak_out[...] = top

        def spread_top(where):
            remote(peak_out, peak_in, top_send, top_recv, where).start()

        others(spread_top, mates)
        peak_in[...] = top

    if mates:

        @pl.when(is_root)
        def _():
            all_received[slot] = message[pl.ds(skip, kept), :]
            own_scale = column_of(scale, skip, kept)
            owners = kept // owned
            total = None
            for f in range(fsdp):
                direct = tops * pair if f < near_levels else dp
                if f == last:
                    drain(all_states.at[pl.ds(0, (dp - pair) * last)], all_state_recv.at[0])
                    place_states(all_column, all_states, owners, False)
                    drain(partial_in, partial_recv)
                    total = total + summed(partial_in, 0, gathered)
                    drain(all_states.at[pl.ds(0, dp - pair)], all_state_recv.at[1])
                    place_states(all_column, all_states, owners, True)
                drain(all_received.at[pl.ds(0, direct - (f == root[1]))], all_recv.at[f])
                more = summed(all_received, f * dp, direct)
                total = more if total is None else total + more
            gradient = total * own_scale
            updated, _, _ = adamw(gradient, all_column[0], all_column[1], all_column[2])
            ready = weights_ref.at[pl.ds(skip, kept)]
            weights_ref[pl.ds(skip, kept), :] = updated.astype(jnp.bfloat16)
            for where in mates[:-1]:
                remote(ready, ready, out_send, out_recv, where).start()

    if mates:

        @pl.when(is_first)
        def _():
            states[pl.ds(seat, 1)] = state[...][None]
            own_scale = column_of(scale, 0, part)
            drain(states.at[pl.ds(0, pair * last - 1)], state_recv.at[0])
            place_states(column, states, pair * fsdp, False)
            drain(states.at[pl.ds(0, pair)], state_recv.at[1])
            place_states(column, states, pair * fsdp, True)
            drain(early_in, early_recv)
            drain(received.at[pl.ds(0, dp)], recv_sems.at[last])
            gradient = (early_in[...] + summed(received, last * dp, dp)) * own_scale
            codes[...] = gradient
            own = (mate[0] * fsdp + mate[1]) * owned
            gradient_in[...] = codes[pl.ds(own, owned), :]
            updated, _, _ = adamw(gradient, column[0], column[1], column[2])
            weights_ref[pl.ds(0, part), :] = updated.astype(jnp.bfloat16)

    def reduce_part(mine, level):
        group = mine // pair if isinstance(mine, int) else lax.div(mine, pair)
        seat = (mine - group * pair) * fsdp + level
        first = group * part
        if not isinstance(first, int):
            first = pl.multiple_of(first, 8)
        received[pl.ds(level * dp + mine, 1)] = message[pl.ds(first, part)][None]
        states[pl.ds(seat, 1)] = state[...][None]
        own_scale = column_of(scale, first, part)
        at_last = proxies[0][1] == last
        total = None
        for f in range(fsdp):
            if f == last:
                if mates and group == 0:
                    early_out[...] = total
                    remote(early_out, early_in, early_send, early_recv, mate).start()
                drain(states.at[pl.ds(0, pair * last - (not at_last))], state_recv.at[0])
                place_states(column, states, pair * fsdp, False)
                drain(states.at[pl.ds(0, pair - at_last)], state_recv.at[1])
                place_states(column, states, pair * fsdp, True)
            own_level = level == f
            run_if(own_level, lambda: drain(received.at[pl.ds(0, dp - 1)], recv_sems.at[f]))
            run_if(negated(own_level), lambda: drain(received.at[pl.ds(0, dp)], recv_sems.at[f]))
            more = summed(received, f * dp, dp)
            total = more if total is None else total + more
        gradient = total * own_scale
        codes[...] = gradient

        def hand_out(at):
            gradient_out[at] = codes[pl.ds(at * owned, owned), :]
            where = (group * pair + at // fsdp, at % fsdp)

            def send():
                remote(gradient_out.at[at], gradient_in, grad_send, grad_recv, where).start()

            run_if(negated(seat == at), send)

        lines_of = pl.ds(first, part)
        ready = weights_ref.at[lines_of]

        def spread(where):
            remote(ready, ready, out_send, out_recv, where).start()

        served = [root] if mates and group == 0 else []
        early = [where[0] * fsdp + where[1] for where in served]
        skipped = [mate[0] * fsdp + mate[1]] if served else []
        late = [at for at in range(pair * fsdp) if at not in early + skipped]
        for at in early if served else late:
            hand_out(at)
        updated, _, _ = adamw(gradient, column[0], column[1], column[2])
        weights_ref[lines_of, :] = updated.astype(jnp.bfloat16)
        for where in served:
            spread(where)
        for at in late if served else early:
            hand_out(at)
        if isinstance(mine, int):
            for where in [(k, f) for k in range(dp) for f in range(fsdp)]:
                if where != (mine, level) and where not in mates:
                    spread(where)
        else:
            others(spread)
        gradient_in[...] = gradient_out[seat]

    if mates:
        for where in proxies:
            pl.when(at_place(where))(functools.partial(reduce_part, *where))
    else:
        pl.when(is_proxy)(functools.partial(reduce_part, mine, level))

    @unless(jnp.logical_or(is_proxy, is_first) if mates else is_proxy)
    def _():
        drain(gradient_in, grad_recv)

    updated, first, second = adamw(gradient_in[...], state[0], state[1], state[2])
    updated_ref[...] = updated
    first_ref[...] = first
    second_ref[...] = second

    @pl.when(is_mate)
    def _():
        peak_in[...] = top_of_all()

    @unless(any_of([is_collector, is_mate]))
    def _():
        drain(peak_in, top_recv)

    for line in range(lines):
        low = line * width
        high = min(low + width, blocks)
        peak_ref[:, low:high] = peak_in[pl.ds(line, 1), : high - low]

    @unless(is_proxy)
    def _():
        drain(message, send_sem)
        drain(state, state_send)

    @pl.when(is_proxy)
    def _():
        drain(message.at[pl.ds(0, (count - 1) * part)], send_sem)

    if mates:

        @unless(jnp.logical_or(is_root, is_idle))
        def _():
            drain(rest, all_send)

        @pl.when(is_kept)
        def _():
            drain(state, all_state_send)

        @pl.when(any_of([at_place(where) for where in combiners]))
        def _():
            drain(partial_out, partial_send)

        @pl.when(at_place(proxies[0]))
        def _():
            drain(early_out, early_send)

        @pl.when(level == last)
        def _():
            drain(message.at[pl.ds(0, part)], far_send)

        @pl.when(jnp.logical_and(group == 0, jnp.logical_not(is_first)))
        def _():
            drain(state, mate_state_send)

    inboxes = len(mates) + 1
    is_inbox = any_of([is_mate, is_collector])

    @pl.when(is_inbox)
    def _():
        if inboxes > 1:
            drain(peak_received.at[pl.ds(0, inboxes - 1)], peak_send)

    @unless(is_inbox)
    def _():
        drain(peak_received.at[pl.ds(0, inboxes)], peak_send)

    @pl.when(is_proxy)
    def _():
        drain(weights_ref.at[pl.ds(0, (count - 1) * part)], out_recv)

    for at, where in enumerate(proxies):

        @pl.when(at_place(where))
        def _():
            unserved = 1 if mates and at == 0 else 0
            drain(gradient_out.at[pl.ds(0, pair * fsdp - 1 - unserved)], grad_send)

    if mates:

        @pl.when(is_root)
        def _():
            drain(weights_ref.at[pl.ds(0, skip)], out_recv)
            for where in mates[:-1]:
                drain(rest, out_send)

        @pl.when(is_first)
        def _():
            drain(rest, out_recv)

        @unless(any_of([is_proxy, is_mate]))
        def _():
            drain(weights_ref, out_recv)

        for at, where in enumerate(proxies):
            reached = n - 1 - (len(mates) if at else 1)

            @pl.when(at_place(where))
            def _():
                drain(received.at[pl.ds(0, reached)], out_send)

    else:

        @unless(is_proxy)
        def _():
            drain(weights_ref, out_recv)

        @pl.when(is_proxy)
        def _():
            drain(received.at[pl.ds(0, n - 1)], out_send)

    @pl.when(is_collector)
    def _():
        drain(peak_received.at[pl.ds(0, n - 1 - len(mates))], top_send)


def finish_kernel(*refs):
    count = (len(refs) - 1) // 2
    sems = refs[-1]
    stores = [
        pltpu.make_async_copy(refs[at], refs[count + at], sems.at[at])
        for at in range(count)
    ]
    for store in stores:
        store.start()
    for store in stores:
        store.wait()


def body(sizes, grads, last_peak, master, moment1, moment2):
    dp, fsdp = sizes
    n = dp * fsdp
    blocks, width = grads.shape[1:]
    pair, proxies, _, mates = layout(sizes, blocks, width)
    count = len(proxies)
    owned = master.shape[0]
    part = blocks // count
    lines = pl.cdiv(blocks, width)
    f32, bf16 = jnp.float32, jnp.bfloat16
    vmem = pl.BlockSpec(memory_space=pltpu.VMEM)
    anywhere = pl.BlockSpec(memory_space=pl.ANY)
    shapes = (
        ((owned, width), f32),
        ((owned, width), f32),
        ((owned, width), f32),
        ((blocks, width), bf16),
        ((1, blocks), f32),
    )
    kept = blocks - part
    near_levels, gathered, _ = gathering(sizes)
    root_scratch = [
        pltpu.VMEM((n, kept, width), bf16),
        pltpu.VMEM((kept // owned, 3, owned, width), f32),
        pltpu.VMEM((3, kept, width), f32),
        pltpu.VMEM((near_levels * pair, kept, width), bf16),
        pltpu.VMEM((kept, width), f32),
        pltpu.VMEM((gathered, kept, width), f32),
        pltpu.SemaphoreType.DMA((fsdp,)),
        pltpu.SemaphoreType.DMA,
        pltpu.SemaphoreType.DMA,
        pltpu.SemaphoreType.DMA((2,)),
        pltpu.SemaphoreType.DMA,
        pltpu.SemaphoreType.DMA,
        pltpu.SemaphoreType.DMA,
        pltpu.VMEM((part, width), f32),
        pltpu.VMEM((part, width), f32),
    ] + [pltpu.SemaphoreType.DMA] * 4
    results = pl.pallas_call(
        functools.partial(kernel, sizes),
        out_shape=tuple(pltpu.VMEM(shape, kind) for shape, kind in shapes),
        in_specs=[anywhere] * 5,
        out_specs=(vmem,) * 5,
        scratch_shapes=[
            pltpu.VMEM((1, blocks, width), f32),
            pltpu.VMEM((1, blocks), f32),
            pltpu.VMEM((3, owned, width), f32),
            pltpu.VMEM((part, width), f32),
            pltpu.VMEM((blocks, width), bf16),
            pltpu.VMEM((n, part, width), bf16),
            pltpu.VMEM((pair * fsdp, 3, owned, width), f32),
            pltpu.VMEM((3, part, width), f32),
            pltpu.VMEM((pair * fsdp, owned, width), f32),
            pltpu.VMEM((owned, width), f32),
            pltpu.VMEM((lines, width), f32),
            pltpu.VMEM((n, lines, width), f32),
            pltpu.VMEM((lines, width), f32),
            pltpu.VMEM((lines, width), f32),
            pltpu.SemaphoreType.DMA((6,)),
            pltpu.SemaphoreType.DMA((fsdp,)),
        ]
        + [pltpu.SemaphoreType.DMA] * 2
        + [pltpu.SemaphoreType.DMA((2,))]
        + [pltpu.SemaphoreType.DMA] * 8
        + (root_scratch if mates else []),
        compiler_params=pltpu.CompilerParams(collective_id=0, has_side_effects=True),
    )(grads, last_peak.reshape(1, blocks), master, moment1, moment2)
    updated, first, second, weights, peak = pl.pallas_call(
        finish_kernel,
        out_shape=tuple(jax.ShapeDtypeStruct(shape, kind) for shape, kind in shapes),
        in_specs=[vmem] * 5,
        out_specs=(anywhere,) * 5,
        scratch_shapes=[pltpu.SemaphoreType.DMA((5,))],
    )(*(pltpu.with_memory_space_constraint(result, pltpu.VMEM) for result in results))
    return (updated, first, second, weights, peak.reshape(blocks))


def solution(mesh):
    sharded = P(AXES, None)
    return jax.shard_map(
        functools.partial(body, (mesh.shape["dp"], mesh.shape["fsdp"])),
        mesh=mesh,
        in_specs=(P(AXES, None, None), P(), sharded, sharded, sharded),
        out_specs=(sharded, sharded, sharded, P(), P()),
        check_vma=False,
    )
```

```python
import functools

import jax
import jax.numpy as jnp
from jax import lax
from jax.experimental import pallas as pl
from jax.experimental.pallas import tpu as pltpu
from jax.sharding import PartitionSpec as P

STEP_COUNT = 10


code_limit = 448.0
peak_floor = 0.05
beta_one = 0.9
beta_two = 0.95
learn_rate = 0.05
decay_rate = 0.1
epsilon = 1e-08
AXES = ("dp", "fsdp")
UNROLL_MOST = 64
ROOT_BYTES = 8 * 2**20


def adamw(gradient, master, moment1, moment2):
    first = beta_one * moment1 + (1.0 - beta_one) * gradient
    second = beta_two * moment2 + (1.0 - beta_two) * gradient * gradient
    corrected_one = first * (1.0 / (1.0 - beta_one**STEP_COUNT))
    corrected_two = second * (1.0 / (1.0 - beta_two**STEP_COUNT))
    updated = master - learn_rate * (
        corrected_one / (jnp.sqrt(corrected_two) + epsilon) + decay_rate * master
    )
    return (updated, first, second)


def layout(sizes, blocks, width):
    dp, fsdp = sizes
    pair = 2 if dp % 2 == 0 else 1
    above = min(1, fsdp - 1)
    proxies = [(pair * q + pair - 1, above) for q in range(dp // pair)]
    collector = (min(3, dp - 1), 0)
    mates = [(k, 0) for k in range(pair)]
    fits = 2 * dp * fsdp * blocks * width <= ROOT_BYTES
    if above == 0 or pair == 1 or dp < 4 * pair or dp % (2 * pair) or not fits:
        mates = []
    return pair, proxies, collector, mates


def gathering(sizes):
    dp, fsdp = sizes
    chips = dp // 2
    count = chips // 4
    return min(2, fsdp - 1), count, [(2 * (g - chips // 2) + 1, 0) for g in range(chips - count, chips)]


def near_root(sizes):
    dp, fsdp = sizes
    return [(3, 0), (dp // 2 + 1, 0)] + [(1, f) for f in range(1, fsdp - 1)]


def kernel(
    sizes,
    grads_hbm,
    last_peak_hbm,
    master_hbm,
    moment1_hbm,
    moment2_hbm,
    updated_ref,
    first_ref,
    second_ref,
    weights_ref,
    peak_ref,
    grads,
    last_peak,
    state,
    codes,
    message,
    received,
    states,
    column,
    gradient_out,
    gradient_in,
    peak_message,
    peak_received,
    peak_out,
    peak_in,
    in_sems,
    recv_sems,
    send_sem,
    state_send,
    state_recv,
    grad_send,
    grad_recv,
    out_send,
    out_recv,
    peak_send,
    peak_recv,
    top_send,
    top_recv,
    *root_refs,
):
    dp, fsdp = sizes
    n = dp * fsdp
    blocks, width = message.shape
    pair, proxies, collector, mates = layout(sizes, blocks, width)
    count = len(proxies)
    hubs = proxies + [collector] + mates
    owned = blocks // n
    part = blocks // count
    lines = peak_out.shape[0]
    mine, level = lax.axis_index("dp"), lax.axis_index("fsdp")
    me = mine * fsdp + level
    slot = level * dp + mine
    group = lax.div(mine, pair)
    seat = lax.rem(mine, pair) * fsdp + level

    def at_place(where):
        return jnp.logical_and(mine == where[0], level == where[1])

    def any_of(flags):
        return functools.reduce(jnp.logical_or, flags, jnp.bool_(False))

    def unless(flag):
        return pl.when(jnp.logical_not(flag))

    is_proxy = any_of([at_place(where) for where in proxies])
    is_collector = at_place(collector)
    is_mate = any_of([at_place(where) for where in mates])
    is_hub = any_of([is_proxy, is_collector, is_mate])
    if mates:
        root = mates[-1]
        is_root = at_place(root)
        skip, kept = part, blocks - part
        rest = message.at[pl.ds(skip, kept)]
        is_kept = me * owned >= skip
        mate = mates[0]
        beside = near_root(sizes)
        is_first = at_place(mate)
        near_levels, gathered, combiners = gathering(sizes)
        tops = dp // pair - gathered
        nears = []
        for at in range(gathered):
            chip = (tops + at) * pair
            nears.append([(k, f) for f in range(near_levels) for k in range(chip, chip + pair)])
        in_nears = [jnp.logical_and(level < near_levels, group == tops + at) for at in range(gathered)]
        is_near = any_of(in_nears)
        idle = [where for where, near in zip(combiners, nears) if where in near]
        is_idle = any_of([at_place(where) for where in idle])
        (
            all_received,
            all_states,
            all_column,
            near_received,
            partial_out,
            partial_in,
            all_recv,
            all_send,
            all_state_send,
            all_state_recv,
            near_recv,
            partial_send,
            partial_recv,
            early_out,
            early_in,
            early_send,
            early_recv,
            far_send,
            mate_state_send,
        ) = root_refs

    def remote(source, target, send, recv, where):
        return pltpu.make_async_remote_copy(
            src_ref=source,
            dst_ref=target,
            send_sem=send,
            recv_sem=recv,
            device_id=where,
            device_id_type=pl.DeviceIdType.MESH,
        )

    def drain(ref, sem):
        pltpu.make_async_copy(ref, ref, sem).wait()

    def others(step, skipped=()):
        if n <= UNROLL_MOST:
            near = [(k, f) for f in range(fsdp) for k in range(pair)]
            far = [(k, f) for f in range(fsdp) for k in range(pair, dp)]
            for where in near + far:
                if where not in skipped:
                    unless(at_place(where))(functools.partial(step, where))
        else:

            def turn(k, carry):
                other = lax.rem(me + k, n)
                step((lax.div(other, fsdp), lax.rem(other, fsdp)))
                return carry

            lax.fori_loop(1, n, turn, 0)

    loads = [
        pltpu.make_async_copy(source, target, in_sems.at[at])
        for at, (source, target) in enumerate(
            (
                (last_peak_hbm, last_peak),
                (grads_hbm.at[:, pl.ds(0, part)], grads.at[:, pl.ds(0, part)]),
                (grads_hbm.at[:, pl.ds(part, blocks - part)], grads.at[:, pl.ds(part, blocks - part)]),
                (master_hbm, state.at[0]),
                (moment1_hbm, state.at[1]),
                (moment2_hbm, state.at[2]),
            )
        )
    ]
    for load in loads:
        load.start()
    barrier = pltpu.get_barrier_semaphore()

    def greet(where):
        pl.semaphore_signal(
            barrier, inc=1, device_id=where, device_id_type=pl.DeviceIdType.MESH
        )

    @pl.when(is_hub)
    def _():
        others(greet)

    if mates:

        for combiner, near in zip(combiners, nears):
            if combiner not in hubs:

                @pl.when(at_place(combiner))
                def _():
                    for where in near:
                        if where != combiner:
                            greet(where)

    loads[0].wait()
    floored = jnp.maximum(last_peak[...], peak_floor)
    inverse = code_limit / floored
    scale = floored / code_limit
    row = lax.broadcasted_iota(jnp.int32, (blocks, blocks), 0)
    lane = lax.broadcasted_iota(jnp.int32, (blocks, blocks), 1)
    diagonal = row == lane
    inverse_column = jnp.sum(jnp.where(diagonal, inverse, 0.0), axis=1, keepdims=True)
    def encode(first, rows):
        scaled = grads[0, pl.ds(first, rows), :] * inverse_column[first : first + rows]
        message[pl.ds(first, rows), :] = jnp.clip(scaled, -code_limit, code_limit).astype(jnp.bfloat16)

    loads[1].wait()
    encode(0, part)

    if mates:
        greeted_more = any_of(
            [flag for flag, combiner in zip(in_nears, combiners) if combiner not in hubs]
        )
        greeted_more = jnp.logical_and(greeted_more, jnp.logical_not(is_idle))
        for flag, more in ((greeted_more, 1), (jnp.logical_not(greeted_more), 0)):

            @pl.when(jnp.logical_and(flag, is_hub))
            def _():
                pl.semaphore_wait(barrier, len(hubs) - 1 + more)

            @pl.when(jnp.logical_and(flag, jnp.logical_not(is_hub)))
            def _():
                pl.semaphore_wait(barrier, len(hubs) + more)

    else:

        @pl.when(is_hub)
        def _():
            pl.semaphore_wait(barrier, len(hubs) - 1)

        @unless(is_hub)
        def _():
            pl.semaphore_wait(barrier, len(hubs))

    last = fsdp - 1
    lateness = lax.div(level, max(last, 1))

    def send_part(q, where):
        @unless(at_place(where))
        def _():
            source = message.at[pl.ds(q * part, part)]
            remote(source, received.at[slot], send_sem, recv_sems.at[level], where).start()

    if mates:

        @pl.when(level == last)
        def _():
            source = message.at[pl.ds(0, part)]
            remote(source, received.at[slot], far_send, recv_sems.at[level], mate).start()

        @unless(level == last)
        def _():
            send_part(0, proxies[0])

    else:
        send_part(0, proxies[0])
    loads[2].wait()
    encode(part, blocks - part)
    values = grads[0]

    if mates:

        @pl.when(level == last)
        def _():
            send_part(0, proxies[0])

        @unless(jnp.logical_or(is_root, is_near))
        def _():
            remote(rest, all_received.at[slot], all_send, all_recv.at[level], root).start()

        for at, combiner in enumerate(combiners):

            @pl.when(jnp.logical_and(in_nears[at], jnp.logical_not(at_place(combiner))))
            def _():
                target = near_received.at[level * pair + mine - (tops + at) * pair]
                remote(rest, target, all_send, near_recv, combiner).start()

    for load in loads[3:]:
        load.wait()
    if mates:

        @pl.when(is_kept)
        def _():
            target = all_states.at[me - skip // owned]
            remote(state, target, all_state_send, all_state_recv.at[lateness], root).start()

        @pl.when(jnp.logical_and(group == 0, jnp.logical_not(is_first)))
        def _():
            target = states.at[seat]
            remote(state, target, mate_state_send, state_recv.at[lateness], mate).start()

    for q, where in enumerate(proxies):

        @pl.when(jnp.logical_and(group == q, jnp.logical_not(is_proxy)))
        def _():
            remote(state, states.at[seat], state_send, state_recv.at[lateness], where).start()

    peak_column = jnp.max(jnp.abs(values), axis=1, keepdims=True)
    peak_row = jnp.max(jnp.where(diagonal, peak_column, 0.0), axis=0, keepdims=True)
    peak_message[...] = jnp.zeros_like(peak_message)
    for line in range(lines):
        low = line * width
        high = min(low + width, blocks)
        peak_message[pl.ds(line, 1), : high - low] = peak_row[:, low:high]

    for where in mates + [collector]:

        @unless(at_place(where))
        def _():
            remote(peak_message, peak_received.at[me], peak_send, peak_recv, where).start()

    for q, where in list(enumerate(proxies))[1:]:
        send_part(q, where)

    def top_of_all():
        peak_received[me] = peak_message[...]
        drain(peak_received.at[pl.ds(0, n - 1)], peak_recv)
        return jnp.max(peak_received[...], axis=0)

    def column_of(values, first, rows):
        at_row = lax.broadcasted_iota(jnp.int32, (rows, blocks), 0)
        at_lane = lax.broadcasted_iota(jnp.int32, (rows, blocks), 1)
        return jnp.sum(jnp.where(at_lane == at_row + first, values, 0.0), axis=1, keepdims=True)

    def run_if(flag, step):
        if isinstance(flag, bool):
            if flag:
                step()
        else:
            pl.when(flag)(step)

    def negated(flag):
        return not flag if isinstance(flag, bool) else jnp.logical_not(flag)

    def place_states(target, source, owners, late):
        for at in range(owners):
            if (at % fsdp == last) == late:
                for kind in range(3):
                    target[kind, pl.ds(at * owned, owned), :] = source[at, kind]

    def summed(inbox, first, rows):
        return jnp.sum(inbox[pl.ds(first, rows)].astype(jnp.float32), axis=0)

    if mates:
        for at, (combiner, near) in enumerate(zip(combiners, nears)):

            @pl.when(at_place(combiner))
            def _():
                own = combiner in near
                if own:
                    near_received[near.index(combiner)] = message[pl.ds(skip, kept), :]
                drain(near_received.at[pl.ds(0, len(near) - own)], near_recv)
                partial_out[...] = summed(near_received, 0, len(near))
                remote(partial_out, partial_in.at[at], partial_send, partial_recv, root).start()

    @pl.when(is_collector)
    def _():
        top = top_of_all()
        peak_out[...] = top

        def spread_top(where):
            remote(peak_out, peak_in, top_send, top_recv, where).start()

        others(spread_top, mates)
        peak_in[...] = top

    if mates:

        @pl.when(is_root)
        def _():
            all_received[slot] = message[pl.ds(skip, kept), :]
            own_scale = column_of(scale, skip, kept)
            owners = kept // owned
            total = None
            for f in range(fsdp):
                direct = tops * pair if f < near_levels else dp
                if f == last:
                    drain(all_states.at[pl.ds(0, (dp - pair) * last)], all_state_recv.at[0])
                    place_states(all_column, all_states, owners, False)
                    drain(partial_in, partial_recv)
                    total = total + summed(partial_in, 0, gathered)
                    drain(all_states.at[pl.ds(0, dp - pair)], all_state_recv.at[1])
                    place_states(all_column, all_states, owners, True)
                drain(all_received.at[pl.ds(0, direct - (f == root[1]))], all_recv.at[f])
                more = summed(all_received, f * dp, direct)
                total = more if total is None else total + more
            gradient = total * own_scale
            updated, _, _ = adamw(gradient, all_column[0], all_column[1], all_column[2])
            ready = weights_ref.at[pl.ds(skip, kept)]
            weights_ref[pl.ds(skip, kept), :] = updated.astype(jnp.bfloat16)
            for where in [mate] + beside:
                remote(ready, ready, out_send, out_recv, where).start()

    if mates:

        @pl.when(is_first)
        def _():
            states[pl.ds(seat, 1)] = state[...][None]
            own_scale = column_of(scale, 0, part)
            drain(states.at[pl.ds(0, pair * last - 1)], state_recv.at[0])
            place_states(column, states, pair * fsdp, False)
            drain(states.at[pl.ds(0, pair)], state_recv.at[1])
            place_states(column, states, pair * fsdp, True)
            drain(early_in, early_recv)
            drain(received.at[pl.ds(0, dp)], recv_sems.at[last])
            gradient = (early_in[...] + summed(received, last * dp, dp)) * own_scale
            codes[...] = gradient
            own = (mate[0] * fsdp + mate[1]) * owned
            gradient_in[...] = codes[pl.ds(own, owned), :]
            updated, _, _ = adamw(gradient, column[0], column[1], column[2])
            weights_ref[pl.ds(0, part), :] = updated.astype(jnp.bfloat16)

    def reduce_part(mine, level):
        group = mine // pair if isinstance(mine, int) else lax.div(mine, pair)
        seat = (mine - group * pair) * fsdp + level
        first = group * part
        if not isinstance(first, int):
            first = pl.multiple_of(first, 8)
        received[pl.ds(level * dp + mine, 1)] = message[pl.ds(first, part)][None]
        states[pl.ds(seat, 1)] = state[...][None]
        own_scale = column_of(scale, first, part)
        at_last = proxies[0][1] == last
        total = None
        for f in range(fsdp):
            if f == last:
                if mates and group == 0:
                    early_out[...] = total
                    remote(early_out, early_in, early_send, early_recv, mate).start()
                drain(states.at[pl.ds(0, pair * last - (not at_last))], state_recv.at[0])
                place_states(column, states, pair * fsdp, False)
                drain(states.at[pl.ds(0, pair - at_last)], state_recv.at[1])
                place_states(column, states, pair * fsdp, True)
            own_level = level == f
            run_if(own_level, lambda: drain(received.at[pl.ds(0, dp - 1)], recv_sems.at[f]))
            run_if(negated(own_level), lambda: drain(received.at[pl.ds(0, dp)], recv_sems.at[f]))
            more = summed(received, f * dp, dp)
            total = more if total is None else total + more
        gradient = total * own_scale
        codes[...] = gradient

        def hand_out(at):
            gradient_out[at] = codes[pl.ds(at * owned, owned), :]
            where = (group * pair + at // fsdp, at % fsdp)

            def send():
                remote(gradient_out.at[at], gradient_in, grad_send, grad_recv, where).start()

            run_if(negated(seat == at), send)

        lines_of = pl.ds(first, part)
        ready = weights_ref.at[lines_of]

        def spread(where):
            remote(ready, ready, out_send, out_recv, where).start()

        served = [root] if mates and group == 0 else []
        early = [where[0] * fsdp + where[1] for where in served]
        skipped = [mate[0] * fsdp + mate[1]] if served else []
        late = [at for at in range(pair * fsdp) if at not in early + skipped]
        for at in early if served else late:
            hand_out(at)
        updated, _, _ = adamw(gradient, column[0], column[1], column[2])
        weights_ref[lines_of, :] = updated.astype(jnp.bfloat16)
        for where in served:
            spread(where)
        for at in late if served else early:
            hand_out(at)
        if isinstance(mine, int):
            unserved = mates if group == 0 else mates + beside
            for where in [(k, f) for k in range(dp) for f in range(fsdp)]:
                if where != (mine, level) and where not in unserved:
                    spread(where)
        else:
            others(spread)
        gradient_in[...] = gradient_out[seat]

    if mates:
        for where in proxies:
            pl.when(at_place(where))(functools.partial(reduce_part, *where))
    else:
        pl.when(is_proxy)(functools.partial(reduce_part, mine, level))

    @unless(jnp.logical_or(is_proxy, is_first) if mates else is_proxy)
    def _():
        drain(gradient_in, grad_recv)

    updated, first, second = adamw(gradient_in[...], state[0], state[1], state[2])
    updated_ref[...] = updated
    first_ref[...] = first
    second_ref[...] = second

    @pl.when(is_mate)
    def _():
        peak_in[...] = top_of_all()

    @unless(any_of([is_collector, is_mate]))
    def _():
        drain(peak_in, top_recv)

    for line in range(lines):
        low = line * width
        high = min(low + width, blocks)
        peak_ref[:, low:high] = peak_in[pl.ds(line, 1), : high - low]

    @unless(is_proxy)
    def _():
        drain(message, send_sem)
        drain(state, state_send)

    @pl.when(is_proxy)
    def _():
        drain(message.at[pl.ds(0, (count - 1) * part)], send_sem)

    if mates:

        @unless(jnp.logical_or(is_root, is_idle))
        def _():
            drain(rest, all_send)

        @pl.when(is_kept)
        def _():
            drain(state, all_state_send)

        @pl.when(any_of([at_place(where) for where in combiners]))
        def _():
            drain(partial_out, partial_send)

        @pl.when(at_place(proxies[0]))
        def _():
            drain(early_out, early_send)

        @pl.when(level == last)
        def _():
            drain(message.at[pl.ds(0, part)], far_send)

        @pl.when(jnp.logical_and(group == 0, jnp.logical_not(is_first)))
        def _():
            drain(state, mate_state_send)

    inboxes = len(mates) + 1
    is_inbox = any_of([is_mate, is_collector])

    @pl.when(is_inbox)
    def _():
        if inboxes > 1:
            drain(peak_received.at[pl.ds(0, inboxes - 1)], peak_send)

    @unless(is_inbox)
    def _():
        drain(peak_received.at[pl.ds(0, inboxes)], peak_send)

    @pl.when(is_proxy)
    def _():
        drain(weights_ref.at[pl.ds(0, (count - 1) * part)], out_recv)

    for at, where in enumerate(proxies):

        @pl.when(at_place(where))
        def _():
            unserved = 1 if mates and at == 0 else 0
            drain(gradient_out.at[pl.ds(0, pair * fsdp - 1 - unserved)], grad_send)

    if mates:

        @pl.when(is_root)
        def _():
            drain(weights_ref.at[pl.ds(0, skip)], out_recv)
            drain(all_received.at[pl.ds(0, 1 + len(beside))], out_send)

        @pl.when(is_first)
        def _():
            drain(rest, out_recv)

        @unless(any_of([is_proxy, is_mate]))
        def _():
            drain(weights_ref, out_recv)

        for at, where in enumerate(proxies):
            reached = n - 1 - (len(mates + beside) if at else 1)

            @pl.when(at_place(where))
            def _():
                drain(received.at[pl.ds(0, reached)], out_send)

    else:

        @unless(is_proxy)
        def _():
            drain(weights_ref, out_recv)

        @pl.when(is_proxy)
        def _():
            drain(received.at[pl.ds(0, n - 1)], out_send)

    @pl.when(is_collector)
    def _():
        drain(peak_received.at[pl.ds(0, n - 1 - len(mates))], top_send)


def finish_kernel(*refs):
    count = (len(refs) - 1) // 2
    sems = refs[-1]
    stores = [
        pltpu.make_async_copy(refs[at], refs[count + at], sems.at[at])
        for at in range(count)
    ]
    for store in stores:
        store.start()
    for store in stores:
        store.wait()


def body(sizes, grads, last_peak, master, moment1, moment2):
    dp, fsdp = sizes
    n = dp * fsdp
    blocks, width = grads.shape[1:]
    pair, proxies, _, mates = layout(sizes, blocks, width)
    count = len(proxies)
    owned = master.shape[0]
    part = blocks // count
    lines = pl.cdiv(blocks, width)
    f32, bf16 = jnp.float32, jnp.bfloat16
    vmem = pl.BlockSpec(memory_space=pltpu.VMEM)
    anywhere = pl.BlockSpec(memory_space=pl.ANY)
    shapes = (
        ((owned, width), f32),
        ((owned, width), f32),
        ((owned, width), f32),
        ((blocks, width), bf16),
        ((1, blocks), f32),
    )
    kept = blocks - part
    near_levels, gathered, _ = gathering(sizes)
    root_scratch = [
        pltpu.VMEM((n, kept, width), bf16),
        pltpu.VMEM((kept // owned, 3, owned, width), f32),
        pltpu.VMEM((3, kept, width), f32),
        pltpu.VMEM((near_levels * pair, kept, width), bf16),
        pltpu.VMEM((kept, width), f32),
        pltpu.VMEM((gathered, kept, width), f32),
        pltpu.SemaphoreType.DMA((fsdp,)),
        pltpu.SemaphoreType.DMA,
        pltpu.SemaphoreType.DMA,
        pltpu.SemaphoreType.DMA((2,)),
        pltpu.SemaphoreType.DMA,
        pltpu.SemaphoreType.DMA,
        pltpu.SemaphoreType.DMA,
        pltpu.VMEM((part, width), f32),
        pltpu.VMEM((part, width), f32),
    ] + [pltpu.SemaphoreType.DMA] * 4
    results = pl.pallas_call(
        functools.partial(kernel, sizes),
        out_shape=tuple(pltpu.VMEM(shape, kind) for shape, kind in shapes),
        in_specs=[anywhere] * 5,
        out_specs=(vmem,) * 5,
        scratch_shapes=[
            pltpu.VMEM((1, blocks, width), f32),
            pltpu.VMEM((1, blocks), f32),
            pltpu.VMEM((3, owned, width), f32),
            pltpu.VMEM((part, width), f32),
            pltpu.VMEM((blocks, width), bf16),
            pltpu.VMEM((n, part, width), bf16),
            pltpu.VMEM((pair * fsdp, 3, owned, width), f32),
            pltpu.VMEM((3, part, width), f32),
            pltpu.VMEM((pair * fsdp, owned, width), f32),
            pltpu.VMEM((owned, width), f32),
            pltpu.VMEM((lines, width), f32),
            pltpu.VMEM((n, lines, width), f32),
            pltpu.VMEM((lines, width), f32),
            pltpu.VMEM((lines, width), f32),
            pltpu.SemaphoreType.DMA((6,)),
            pltpu.SemaphoreType.DMA((fsdp,)),
        ]
        + [pltpu.SemaphoreType.DMA] * 2
        + [pltpu.SemaphoreType.DMA((2,))]
        + [pltpu.SemaphoreType.DMA] * 8
        + (root_scratch if mates else []),
        compiler_params=pltpu.CompilerParams(collective_id=0, has_side_effects=True),
    )(grads, last_peak.reshape(1, blocks), master, moment1, moment2)
    updated, first, second, weights, peak = pl.pallas_call(
        finish_kernel,
        out_shape=tuple(jax.ShapeDtypeStruct(shape, kind) for shape, kind in shapes),
        in_specs=[vmem] * 5,
        out_specs=(anywhere,) * 5,
        scratch_shapes=[pltpu.SemaphoreType.DMA((5,))],
    )(*(pltpu.with_memory_space_constraint(result, pltpu.VMEM) for result in results))
    return (updated, first, second, weights, peak.reshape(blocks))


def solution(mesh):
    sharded = P(AXES, None)
    return jax.shard_map(
        functools.partial(body, (mesh.shape["dp"], mesh.shape["fsdp"])),
        mesh=mesh,
        in_specs=(P(AXES, None, None), P(), sharded, sharded, sharded),
        out_specs=(sharded, sharded, sharded, P(), P()),
        check_vma=False,
    )
```

```python
import functools

import jax
import jax.numpy as jnp
from jax import lax
from jax.experimental import pallas as pl
from jax.experimental.pallas import tpu as pltpu
from jax.sharding import PartitionSpec as P

STEP_COUNT = 10


code_limit = 448.0
peak_floor = 0.05
beta_one = 0.9
beta_two = 0.95
learn_rate = 0.05
decay_rate = 0.1
epsilon = 1e-08
AXES = ("dp", "fsdp")
UNROLL_MOST = 64
ROOT_BYTES = 8 * 2**20


def adamw(gradient, master, moment1, moment2):
    first = beta_one * moment1 + (1.0 - beta_one) * gradient
    second = beta_two * moment2 + (1.0 - beta_two) * gradient * gradient
    corrected_one = first * (1.0 / (1.0 - beta_one**STEP_COUNT))
    corrected_two = second * (1.0 / (1.0 - beta_two**STEP_COUNT))
    updated = master - learn_rate * (
        corrected_one / (jnp.sqrt(corrected_two) + epsilon) + decay_rate * master
    )
    return (updated, first, second)


def layout(sizes, blocks, width):
    dp, fsdp = sizes
    pair = 2 if dp % 2 == 0 else 1
    above = min(1, fsdp - 1)
    proxies = [(pair * q + pair - 1, above) for q in range(dp // pair)]
    collector = (min(3, dp - 1), 0)
    mates = [(k, 0) for k in range(pair)]
    fits = 2 * dp * fsdp * blocks * width <= ROOT_BYTES
    if above == 0 or pair == 1 or dp < 4 * pair or dp % (2 * pair) or not fits:
        mates = []
    return pair, proxies, collector, mates


def gathering(sizes):
    dp, fsdp = sizes
    chips = dp // 2
    count = chips // 4
    return min(2, fsdp - 1), count, [(2 * (g - chips // 2) + 1, 0) for g in range(chips - count, chips)]


def near_root(sizes):
    dp, fsdp = sizes
    return [(3, 0), (dp // 2 + 1, 0)] + [(1, f) for f in range(1, fsdp - 1)]


def kernel(
    sizes,
    grads_hbm,
    last_peak_hbm,
    master_hbm,
    moment1_hbm,
    moment2_hbm,
    updated_ref,
    first_ref,
    second_ref,
    weights_ref,
    peak_ref,
    grads,
    last_peak,
    state,
    codes,
    message,
    received,
    states,
    column,
    gradient_out,
    gradient_in,
    peak_message,
    peak_received,
    peak_out,
    peak_in,
    in_sems,
    recv_sems,
    send_sem,
    state_send,
    state_recv,
    grad_send,
    grad_recv,
    out_send,
    out_recv,
    peak_send,
    peak_recv,
    top_send,
    top_recv,
    *root_refs,
):
    dp, fsdp = sizes
    n = dp * fsdp
    blocks, width = message.shape
    pair, proxies, collector, mates = layout(sizes, blocks, width)
    count = len(proxies)
    hubs = proxies + [collector] + mates
    owned = blocks // n
    part = blocks // count
    lines = peak_out.shape[0]
    mine, level = lax.axis_index("dp"), lax.axis_index("fsdp")
    me = mine * fsdp + level
    slot = level * dp + mine
    group = lax.div(mine, pair)
    seat = lax.rem(mine, pair) * fsdp + level

    def at_place(where):
        return jnp.logical_and(mine == where[0], level == where[1])

    def any_of(flags):
        return functools.reduce(jnp.logical_or, flags, jnp.bool_(False))

    def unless(flag):
        return pl.when(jnp.logical_not(flag))

    is_proxy = any_of([at_place(where) for where in proxies])
    is_collector = at_place(collector)
    is_mate = any_of([at_place(where) for where in mates])
    is_hub = any_of([is_proxy, is_collector, is_mate])
    if mates:
        root = mates[-1]
        is_root = at_place(root)
        skip, kept = part, blocks - part
        rest = message.at[pl.ds(skip, kept)]
        is_kept = me * owned >= skip
        mate = mates[0]
        beside = near_root(sizes)
        is_first = at_place(mate)
        near_levels, gathered, combiners = gathering(sizes)
        tops = dp // pair - gathered
        nears = []
        for at in range(gathered):
            chip = (tops + at) * pair
            nears.append([(k, f) for f in range(near_levels) for k in range(chip, chip + pair)])
        in_nears = [jnp.logical_and(level < near_levels, group == tops + at) for at in range(gathered)]
        is_near = any_of(in_nears)
        idle = [where for where, near in zip(combiners, nears) if where in near]
        is_idle = any_of([at_place(where) for where in idle])
        (
            all_received,
            all_states,
            all_column,
            near_received,
            partial_out,
            partial_in,
            early_out,
            early_in,
        ) = root_refs
        near_recv = recv_sems.at[0]

    def remote(source, target, send, recv, where):
        return pltpu.make_async_remote_copy(
            src_ref=source,
            dst_ref=target,
            send_sem=send,
            recv_sem=recv,
            device_id=where,
            device_id_type=pl.DeviceIdType.MESH,
        )

    def drain(ref, sem):
        pltpu.make_async_copy(ref, ref, sem).wait()

    def others(step, skipped=()):
        if n <= UNROLL_MOST:
            near = [(k, f) for f in range(fsdp) for k in range(pair)]
            far = [(k, f) for f in range(fsdp) for k in range(pair, dp)]
            for where in near + far:
                if where not in skipped:
                    unless(at_place(where))(functools.partial(step, where))
        else:

            def turn(k, carry):
                other = lax.rem(me + k, n)
                step((lax.div(other, fsdp), lax.rem(other, fsdp)))
                return carry

            lax.fori_loop(1, n, turn, 0)

    loads = [
        pltpu.make_async_copy(source, target, in_sems.at[min(at, 3)])
        for at, (source, target) in enumerate(
            (
                (last_peak_hbm, last_peak),
                (grads_hbm.at[:, pl.ds(0, part)], grads.at[:, pl.ds(0, part)]),
                (grads_hbm.at[:, pl.ds(part, blocks - part)], grads.at[:, pl.ds(part, blocks - part)]),
                (master_hbm, state.at[0]),
                (moment1_hbm, state.at[1]),
                (moment2_hbm, state.at[2]),
            )
        )
    ]
    for load in loads:
        load.start()
    barrier = pltpu.get_barrier_semaphore()

    def greet(where):
        pl.semaphore_signal(
            barrier, inc=1, device_id=where, device_id_type=pl.DeviceIdType.MESH
        )

    @pl.when(is_hub)
    def _():
        others(greet)

    if mates:

        for combiner, near in zip(combiners, nears):
            if combiner not in hubs:

                @pl.when(at_place(combiner))
                def _():
                    for where in near:
                        if where != combiner:
                            greet(where)

    loads[0].wait()
    floored = jnp.maximum(last_peak[...], peak_floor)
    inverse = code_limit / floored
    scale = floored / code_limit
    row = lax.broadcasted_iota(jnp.int32, (blocks, blocks), 0)
    lane = lax.broadcasted_iota(jnp.int32, (blocks, blocks), 1)
    diagonal = row == lane
    inverse_column = jnp.sum(jnp.where(diagonal, inverse, 0.0), axis=1, keepdims=True)
    def encode(first, rows):
        scaled = grads[0, pl.ds(first, rows), :] * inverse_column[first : first + rows]
        message[pl.ds(first, rows), :] = jnp.clip(scaled, -code_limit, code_limit).astype(jnp.bfloat16)

    loads[1].wait()
    encode(0, part)

    if mates:
        greeted_more = any_of(
            [flag for flag, combiner in zip(in_nears, combiners) if combiner not in hubs]
        )
        greeted_more = jnp.logical_and(greeted_more, jnp.logical_not(is_idle))
        for flag, more in ((greeted_more, 1), (jnp.logical_not(greeted_more), 0)):

            @pl.when(jnp.logical_and(flag, is_hub))
            def _():
                pl.semaphore_wait(barrier, len(hubs) - 1 + more)

            @pl.when(jnp.logical_and(flag, jnp.logical_not(is_hub)))
            def _():
                pl.semaphore_wait(barrier, len(hubs) + more)

    else:

        @pl.when(is_hub)
        def _():
            pl.semaphore_wait(barrier, len(hubs) - 1)

        @unless(is_hub)
        def _():
            pl.semaphore_wait(barrier, len(hubs))

    last = fsdp - 1
    lateness = lax.div(level, max(last, 1))

    def send_part(q, where):
        @unless(at_place(where))
        def _():
            source = message.at[pl.ds(q * part, part)]
            remote(source, received.at[slot], send_sem, recv_sems.at[level], where).start()

    if mates:

        @pl.when(level == last)
        def _():
            source = message.at[pl.ds(0, part)]
            remote(source, received.at[slot], send_sem, recv_sems.at[level], mate).start()

        @unless(level == last)
        def _():
            send_part(0, proxies[0])

    else:
        send_part(0, proxies[0])
    loads[2].wait()
    encode(part, blocks - part)
    values = grads[0]

    if mates:

        @pl.when(level == last)
        def _():
            send_part(0, proxies[0])

        @unless(jnp.logical_or(is_root, is_near))
        def _():
            remote(rest, all_received.at[slot], send_sem, recv_sems.at[level], root).start()

        for at, combiner in enumerate(combiners):

            @pl.when(jnp.logical_and(in_nears[at], jnp.logical_not(at_place(combiner))))
            def _():
                target = near_received.at[level * pair + mine - (tops + at) * pair]
                remote(rest, target, send_sem, near_recv, combiner).start()

    drain(state, in_sems.at[3])
    if mates:

        @pl.when(is_kept)
        def _():
            target = all_states.at[me - skip // owned]
            remote(state, target, state_send, state_recv.at[lateness], root).start()

        @pl.when(jnp.logical_and(group == 0, jnp.logical_not(is_first)))
        def _():
            target = states.at[seat]
            remote(state, target, state_send, state_recv.at[lateness], mate).start()

    for q, where in enumerate(proxies):

        @pl.when(jnp.logical_and(group == q, jnp.logical_not(is_proxy)))
        def _():
            remote(state, states.at[seat], state_send, state_recv.at[lateness], where).start()

    peak_column = jnp.max(jnp.abs(values), axis=1, keepdims=True)
    peak_row = jnp.max(jnp.where(diagonal, peak_column, 0.0), axis=0, keepdims=True)
    peak_message[...] = jnp.zeros_like(peak_message)
    for line in range(lines):
        low = line * width
        high = min(low + width, blocks)
        peak_message[pl.ds(line, 1), : high - low] = peak_row[:, low:high]

    for where in mates + [collector]:

        @unless(at_place(where))
        def _():
            remote(peak_message, peak_received.at[me], peak_send, peak_recv, where).start()

    for q, where in list(enumerate(proxies))[1:]:
        send_part(q, where)

    def top_of_all():
        peak_received[me] = peak_message[...]
        drain(peak_received.at[pl.ds(0, n - 1)], peak_recv)
        return jnp.max(peak_received[...], axis=0)

    def column_of(values, first, rows):
        at_row = lax.broadcasted_iota(jnp.int32, (rows, blocks), 0)
        at_lane = lax.broadcasted_iota(jnp.int32, (rows, blocks), 1)
        return jnp.sum(jnp.where(at_lane == at_row + first, values, 0.0), axis=1, keepdims=True)

    def run_if(flag, step):
        if isinstance(flag, bool):
            if flag:
                step()
        else:
            pl.when(flag)(step)

    def negated(flag):
        return not flag if isinstance(flag, bool) else jnp.logical_not(flag)

    def place_states(target, source, owners, late):
        for at in range(owners):
            if (at % fsdp == last) == late:
                for kind in range(3):
                    target[kind, pl.ds(at * owned, owned), :] = source[at, kind]

    def summed(inbox, first, rows):
        return jnp.sum(inbox[pl.ds(first, rows)].astype(jnp.float32), axis=0)

    if mates:
        for at, (combiner, near) in enumerate(zip(combiners, nears)):

            @pl.when(at_place(combiner))
            def _():
                own = combiner in near
                if own:
                    near_received[near.index(combiner)] = message[pl.ds(skip, kept), :]
                drain(near_received.at[pl.ds(0, len(near) - own)], near_recv)
                partial_out[...] = summed(near_received, 0, len(near))
                remote(partial_out, partial_in.at[at], grad_send, top_recv, root).start()

    @pl.when(is_collector)
    def _():
        top = top_of_all()
        peak_out[...] = top

        def spread_top(where):
            remote(peak_out, peak_in, top_send, top_recv, where).start()

        others(spread_top, mates)
        peak_in[...] = top

    if mates:

        @pl.when(is_root)
        def _():
            all_received[slot] = message[pl.ds(skip, kept), :]
            own_scale = column_of(scale, skip, kept)
            owners = kept // owned
            total = None
            for f in range(fsdp):
                direct = tops * pair if f < near_levels else dp
                if f == last:
                    drain(all_states.at[pl.ds(0, (dp - pair) * last)], state_recv.at[0])
                    place_states(all_column, all_states, owners, False)
                    drain(partial_in, top_recv)
                    total = total + summed(partial_in, 0, gathered)
                    drain(all_states.at[pl.ds(0, dp - pair)], state_recv.at[1])
                    place_states(all_column, all_states, owners, True)
                drain(all_received.at[pl.ds(0, direct - (f == root[1]))], recv_sems.at[f])
                more = summed(all_received, f * dp, direct)
                total = more if total is None else total + more
            gradient = total * own_scale
            updated, _, _ = adamw(gradient, all_column[0], all_column[1], all_column[2])
            ready = weights_ref.at[pl.ds(skip, kept)]
            weights_ref[pl.ds(skip, kept), :] = updated.astype(jnp.bfloat16)
            for where in [mate] + beside:
                remote(ready, ready, out_send, out_recv, where).start()

    if mates:

        @pl.when(is_first)
        def _():
            states[pl.ds(seat, 1)] = state[...][None]
            own_scale = column_of(scale, 0, part)
            drain(states.at[pl.ds(0, pair * last - 1)], state_recv.at[0])
            place_states(column, states, pair * fsdp, False)
            drain(states.at[pl.ds(0, pair)], state_recv.at[1])
            place_states(column, states, pair * fsdp, True)
            drain(early_in, top_recv)
            drain(received.at[pl.ds(0, dp)], recv_sems.at[last])
            gradient = (early_in[...] + summed(received, last * dp, dp)) * own_scale
            codes[...] = gradient
            own = (mate[0] * fsdp + mate[1]) * owned
            gradient_in[...] = codes[pl.ds(own, owned), :]
            updated, _, _ = adamw(gradient, column[0], column[1], column[2])
            weights_ref[pl.ds(0, part), :] = updated.astype(jnp.bfloat16)

    def reduce_part(mine, level):
        group = mine // pair if isinstance(mine, int) else lax.div(mine, pair)
        seat = (mine - group * pair) * fsdp + level
        first = group * part
        if not isinstance(first, int):
            first = pl.multiple_of(first, 8)
        received[pl.ds(level * dp + mine, 1)] = message[pl.ds(first, part)][None]
        states[pl.ds(seat, 1)] = state[...][None]
        own_scale = column_of(scale, first, part)
        at_last = proxies[0][1] == last
        total = None
        for f in range(fsdp):
            if f == last:
                if mates and group == 0:
                    early_out[...] = total
                    remote(early_out, early_in, top_send, top_recv, mate).start()
                drain(states.at[pl.ds(0, pair * last - (not at_last))], state_recv.at[0])
                place_states(column, states, pair * fsdp, False)
                drain(states.at[pl.ds(0, pair - at_last)], state_recv.at[1])
                place_states(column, states, pair * fsdp, True)
            own_level = level == f
            run_if(own_level, lambda: drain(received.at[pl.ds(0, dp - 1)], recv_sems.at[f]))
            run_if(negated(own_level), lambda: drain(received.at[pl.ds(0, dp)], recv_sems.at[f]))
            more = summed(received, f * dp, dp)
            total = more if total is None else total + more
        gradient = total * own_scale
        codes[...] = gradient

        def hand_out(at):
            gradient_out[at] = codes[pl.ds(at * owned, owned), :]
            where = (group * pair + at // fsdp, at % fsdp)

            def send():
                remote(gradient_out.at[at], gradient_in, grad_send, grad_recv, where).start()

            run_if(negated(seat == at), send)

        lines_of = pl.ds(first, part)
        ready = weights_ref.at[lines_of]

        def spread(where):
            remote(ready, ready, out_send, out_recv, where).start()

        served = [root] if mates and group == 0 else []
        early = [where[0] * fsdp + where[1] for where in served]
        skipped = [mate[0] * fsdp + mate[1]] if served else []
        late = [at for at in range(pair * fsdp) if at not in early + skipped]
        for at in early if served else late:
            hand_out(at)
        updated, _, _ = adamw(gradient, column[0], column[1], column[2])
        weights_ref[lines_of, :] = updated.astype(jnp.bfloat16)
        for where in served:
            spread(where)
        for at in late if served else early:
            hand_out(at)
        if isinstance(mine, int):
            unserved = mates if group == 0 else mates + beside
            for where in [(k, f) for k in range(dp) for f in range(fsdp)]:
                if where != (mine, level) and where not in unserved:
                    spread(where)
        else:
            others(spread)
        gradient_in[...] = gradient_out[seat]

    if mates:
        for where in proxies:
            pl.when(at_place(where))(functools.partial(reduce_part, *where))
    else:
        pl.when(is_proxy)(functools.partial(reduce_part, mine, level))

    @unless(jnp.logical_or(is_proxy, is_first) if mates else is_proxy)
    def _():
        drain(gradient_in, grad_recv)

    updated, first, second = adamw(gradient_in[...], state[0], state[1], state[2])
    updated_ref[...] = updated
    first_ref[...] = first
    second_ref[...] = second

    @pl.when(is_mate)
    def _():
        peak_in[...] = top_of_all()

    @unless(any_of([is_collector, is_mate]))
    def _():
        drain(peak_in, top_recv)

    for line in range(lines):
        low = line * width
        high = min(low + width, blocks)
        peak_ref[:, low:high] = peak_in[pl.ds(line, 1), : high - low]

    def tally(flags):
        return sum(jnp.where(flag, 1, 0) for flag in flags)

    def drain_first(ref, sem, number, most):
        for value in range(1, most + 1):

            @pl.when(number == value)
            def _():
                drain(ref.at[pl.ds(0, value)], sem)

    parts_sent = count - tally([is_proxy])
    states_sent = tally([jnp.logical_not(is_proxy)])
    if mates:
        parts_sent += (count - 1) * tally([jnp.logical_not(jnp.logical_or(is_root, is_idle))])
        parts_sent += tally([level == last])
        states_sent += tally([is_kept, jnp.logical_and(group == 0, jnp.logical_not(is_first))])
        drain_first(received, send_sem, parts_sent, 2 * count)
        drain_first(states, state_send, states_sent, 3)

        @pl.when(any_of([at_place(where) for where in combiners]))
        def _():
            drain(partial_out, grad_send)

        @pl.when(at_place(proxies[0]))
        def _():
            drain(early_out, top_send)

    else:

        @unless(is_proxy)
        def _():
            drain(message, send_sem)
            drain(state, state_send)

        @pl.when(is_proxy)
        def _():
            drain(message.at[pl.ds(0, (count - 1) * part)], send_sem)

    inboxes = len(mates) + 1
    is_inbox = any_of([is_mate, is_collector])

    @pl.when(is_inbox)
    def _():
        if inboxes > 1:
            drain(peak_received.at[pl.ds(0, inboxes - 1)], peak_send)

    @unless(is_inbox)
    def _():
        drain(peak_received.at[pl.ds(0, inboxes)], peak_send)

    @pl.when(is_proxy)
    def _():
        drain(weights_ref.at[pl.ds(0, (count - 1) * part)], out_recv)

    for at, where in enumerate(proxies):

        @pl.when(at_place(where))
        def _():
            unserved = 1 if mates and at == 0 else 0
            drain(gradient_out.at[pl.ds(0, pair * fsdp - 1 - unserved)], grad_send)

    if mates:

        @pl.when(is_root)
        def _():
            drain(weights_ref.at[pl.ds(0, skip)], out_recv)
            drain(all_received.at[pl.ds(0, 1 + len(beside))], out_send)

        @pl.when(is_first)
        def _():
            drain(rest, out_recv)

        @unless(any_of([is_proxy, is_mate]))
        def _():
            drain(weights_ref, out_recv)

        for at, where in enumerate(proxies):
            reached = n - 1 - (len(mates + beside) if at else 1)

            @pl.when(at_place(where))
            def _():
                drain(received.at[pl.ds(0, reached)], out_send)

    else:

        @unless(is_proxy)
        def _():
            drain(weights_ref, out_recv)

        @pl.when(is_proxy)
        def _():
            drain(received.at[pl.ds(0, n - 1)], out_send)

    @pl.when(is_collector)
    def _():
        drain(peak_received.at[pl.ds(0, n - 1 - len(mates))], top_send)


def finish_kernel(*refs):
    *refs, three, sems = refs
    count = len(refs) // 2
    stores = [
        pltpu.make_async_copy(refs[at], refs[count + at], sems.at[max(at - 2, 0)])
        for at in range(count)
    ]
    for store in stores:
        store.start()
    pltpu.make_async_copy(three, three, sems.at[0]).wait()
    for store in stores[3:]:
        store.wait()


def body(sizes, grads, last_peak, master, moment1, moment2):
    dp, fsdp = sizes
    n = dp * fsdp
    blocks, width = grads.shape[1:]
    pair, proxies, _, mates = layout(sizes, blocks, width)
    count = len(proxies)
    owned = master.shape[0]
    part = blocks // count
    lines = pl.cdiv(blocks, width)
    f32, bf16 = jnp.float32, jnp.bfloat16
    vmem = pl.BlockSpec(memory_space=pltpu.VMEM)
    anywhere = pl.BlockSpec(memory_space=pl.ANY)
    shapes = (
        ((owned, width), f32),
        ((owned, width), f32),
        ((owned, width), f32),
        ((blocks, width), bf16),
        ((1, blocks), f32),
    )
    kept = blocks - part
    near_levels, gathered, _ = gathering(sizes)
    root_scratch = [
        pltpu.VMEM((n, kept, width), bf16),
        pltpu.VMEM((kept // owned, 3, owned, width), f32),
        pltpu.VMEM((3, kept, width), f32),
        pltpu.VMEM((near_levels * pair, kept, width), bf16),
        pltpu.VMEM((kept, width), f32),
        pltpu.VMEM((gathered, kept, width), f32),
        pltpu.VMEM((part, width), f32),
        pltpu.VMEM((part, width), f32),
    ]
    results = pl.pallas_call(
        functools.partial(kernel, sizes),
        out_shape=tuple(pltpu.VMEM(shape, kind) for shape, kind in shapes),
        in_specs=[anywhere] * 5,
        out_specs=(vmem,) * 5,
        scratch_shapes=[
            pltpu.VMEM((1, blocks, width), f32),
            pltpu.VMEM((1, blocks), f32),
            pltpu.VMEM((3, owned, width), f32),
            pltpu.VMEM((part, width), f32),
            pltpu.VMEM((blocks, width), bf16),
            pltpu.VMEM((n, part, width), bf16),
            pltpu.VMEM((pair * fsdp, 3, owned, width), f32),
            pltpu.VMEM((3, part, width), f32),
            pltpu.VMEM((pair * fsdp, owned, width), f32),
            pltpu.VMEM((owned, width), f32),
            pltpu.VMEM((lines, width), f32),
            pltpu.VMEM((n, lines, width), f32),
            pltpu.VMEM((lines, width), f32),
            pltpu.VMEM((lines, width), f32),
            pltpu.SemaphoreType.DMA((4,)),
            pltpu.SemaphoreType.DMA((fsdp,)),
        ]
        + [pltpu.SemaphoreType.DMA] * 2
        + [pltpu.SemaphoreType.DMA((2,))]
        + [pltpu.SemaphoreType.DMA] * 8
        + (root_scratch if mates else []),
        compiler_params=pltpu.CompilerParams(collective_id=0, has_side_effects=True),
    )(grads, last_peak.reshape(1, blocks), master, moment1, moment2)
    updated, first, second, weights, peak = pl.pallas_call(
        finish_kernel,
        out_shape=tuple(jax.ShapeDtypeStruct(shape, kind) for shape, kind in shapes),
        in_specs=[vmem] * 5,
        out_specs=(anywhere,) * 5,
        scratch_shapes=[pltpu.VMEM((3, owned, width), f32), pltpu.SemaphoreType.DMA((3,))],
    )(*(pltpu.with_memory_space_constraint(result, pltpu.VMEM) for result in results))
    return (updated, first, second, weights, peak.reshape(blocks))


def solution(mesh):
    sharded = P(AXES, None)
    return jax.shard_map(
        functools.partial(body, (mesh.shape["dp"], mesh.shape["fsdp"])),
        mesh=mesh,
        in_specs=(P(AXES, None, None), P(), sharded, sharded, sharded),
        out_specs=(sharded, sharded, sharded, P(), P()),
        check_vma=False,
    )
```

```python
import functools

import jax
import jax.numpy as jnp
from jax import lax
from jax.experimental import pallas as pl
from jax.experimental.pallas import tpu as pltpu
from jax.sharding import PartitionSpec as P

STEP_COUNT = 10


code_limit = 448.0
peak_floor = 0.05
beta_one = 0.9
beta_two = 0.95
learn_rate = 0.05
decay_rate = 0.1
epsilon = 1e-08
AXES = ("dp", "fsdp")
UNROLL_MOST = 64
ROOT_BYTES = 8 * 2**20


def adamw(gradient, master, moment1, moment2):
    first = beta_one * moment1 + (1.0 - beta_one) * gradient
    second = beta_two * moment2 + (1.0 - beta_two) * gradient * gradient
    corrected_one = first * (1.0 / (1.0 - beta_one**STEP_COUNT))
    corrected_two = second * (1.0 / (1.0 - beta_two**STEP_COUNT))
    updated = master - learn_rate * (
        corrected_one / (jnp.sqrt(corrected_two) + epsilon) + decay_rate * master
    )
    return (updated, first, second)


def layout(sizes, blocks, width):
    dp, fsdp = sizes
    pair = 2 if dp % 2 == 0 else 1
    above = min(1, fsdp - 1)
    proxies = [(pair * q + pair - 1, above) for q in range(dp // pair)]
    collector = (min(3, dp - 1), 0)
    mates = [(k, 0) for k in range(pair)]
    fits = 2 * dp * fsdp * blocks * width <= ROOT_BYTES
    if above == 0 or pair == 1 or dp < 4 * pair or dp % (2 * pair) or not fits:
        mates = []
    return pair, proxies, collector, mates


def gathering(sizes):
    dp, fsdp = sizes
    chips = dp // 2
    count = chips // 4
    return min(2, fsdp - 1), count, [(2 * (g - chips // 2) + 1, 0) for g in range(chips - count, chips)]


def near_root(sizes):
    dp, fsdp = sizes
    return [(3, 0), (dp // 2 + 1, 0)] + [(1, f) for f in range(1, fsdp - 1)]


def kernel(
    sizes,
    grads_hbm,
    last_peak_hbm,
    master_hbm,
    moment1_hbm,
    moment2_hbm,
    updated_ref,
    first_ref,
    second_ref,
    weights_ref,
    peak_ref,
    grads,
    last_peak,
    state,
    codes,
    message,
    received,
    states,
    column,
    gradient_out,
    gradient_in,
    peak_message,
    peak_received,
    peak_out,
    peak_in,
    in_sems,
    recv_sems,
    send_sem,
    state_send,
    state_recv,
    grad_send,
    grad_recv,
    out_recv,
    peak_send,
    peak_recv,
    top_recv,
    *root_refs,
):
    dp, fsdp = sizes
    n = dp * fsdp
    blocks, width = message.shape
    pair, proxies, collector, mates = layout(sizes, blocks, width)
    count = len(proxies)
    hubs = proxies + [collector] + mates
    owned = blocks // n
    part = blocks // count
    lines = peak_out.shape[0]
    mine, level = lax.axis_index("dp"), lax.axis_index("fsdp")
    me = mine * fsdp + level
    slot = level * dp + mine
    group = lax.div(mine, pair)
    seat = lax.rem(mine, pair) * fsdp + level

    def at_place(where):
        return jnp.logical_and(mine == where[0], level == where[1])

    def any_of(flags):
        return functools.reduce(jnp.logical_or, flags, jnp.bool_(False))

    def unless(flag):
        return pl.when(jnp.logical_not(flag))

    is_proxy = any_of([at_place(where) for where in proxies])
    is_collector = at_place(collector)
    is_mate = any_of([at_place(where) for where in mates])
    is_hub = any_of([is_proxy, is_collector, is_mate])
    if mates:
        root = mates[-1]
        is_root = at_place(root)
        skip, kept = part, blocks - part
        rest = message.at[pl.ds(skip, kept)]
        is_kept = me * owned >= skip
        mate = mates[0]
        beside = near_root(sizes)
        is_first = at_place(mate)
        near_levels, gathered, combiners = gathering(sizes)
        tops = dp // pair - gathered
        nears = []
        for at in range(gathered):
            chip = (tops + at) * pair
            nears.append([(k, f) for f in range(near_levels) for k in range(chip, chip + pair)])
        in_nears = [jnp.logical_and(level < near_levels, group == tops + at) for at in range(gathered)]
        is_near = any_of(in_nears)
        idle = [where for where, near in zip(combiners, nears) if where in near]
        is_idle = any_of([at_place(where) for where in idle])
        (
            all_received,
            all_states,
            all_column,
            near_received,
            partial_out,
            partial_in,
            early_out,
            early_in,
        ) = root_refs
        out_send = send_sem
        near_recv = recv_sems.at[0]
    else:
        (out_send,) = root_refs

    def remote(source, target, send, recv, where):
        return pltpu.make_async_remote_copy(
            src_ref=source,
            dst_ref=target,
            send_sem=send,
            recv_sem=recv,
            device_id=where,
            device_id_type=pl.DeviceIdType.MESH,
        )

    def drain(ref, sem):
        pltpu.make_async_copy(ref, ref, sem).wait()

    def others(step, skipped=()):
        if n <= UNROLL_MOST:
            near = [(k, f) for f in range(fsdp) for k in range(pair)]
            far = [(k, f) for f in range(fsdp) for k in range(pair, dp)]
            for where in near + far:
                if where not in skipped:
                    unless(at_place(where))(functools.partial(step, where))
        else:

            def turn(k, carry):
                other = lax.rem(me + k, n)
                step((lax.div(other, fsdp), lax.rem(other, fsdp)))
                return carry

            lax.fori_loop(1, n, turn, 0)

    loads = [
        pltpu.make_async_copy(source, target, in_sems.at[min(at, 3)])
        for at, (source, target) in enumerate(
            (
                (last_peak_hbm, last_peak),
                (grads_hbm.at[:, pl.ds(0, part)], grads.at[:, pl.ds(0, part)]),
                (grads_hbm.at[:, pl.ds(part, blocks - part)], grads.at[:, pl.ds(part, blocks - part)]),
                (master_hbm, state.at[0]),
                (moment1_hbm, state.at[1]),
                (moment2_hbm, state.at[2]),
            )
        )
    ]
    for load in loads:
        load.start()
    barrier = pltpu.get_barrier_semaphore()

    def greet(where):
        pl.semaphore_signal(
            barrier, inc=1, device_id=where, device_id_type=pl.DeviceIdType.MESH
        )

    @pl.when(is_hub)
    def _():
        others(greet)

    if mates:

        for combiner, near in zip(combiners, nears):
            if combiner not in hubs:

                @pl.when(at_place(combiner))
                def _():
                    for where in near:
                        if where != combiner:
                            greet(where)

    loads[0].wait()
    floored = jnp.maximum(last_peak[...], peak_floor)
    inverse = code_limit / floored
    scale = floored / code_limit
    row = lax.broadcasted_iota(jnp.int32, (blocks, blocks), 0)
    lane = lax.broadcasted_iota(jnp.int32, (blocks, blocks), 1)
    diagonal = row == lane
    inverse_column = jnp.sum(jnp.where(diagonal, inverse, 0.0), axis=1, keepdims=True)
    def encode(first, rows):
        scaled = grads[0, pl.ds(first, rows), :] * inverse_column[first : first + rows]
        message[pl.ds(first, rows), :] = jnp.clip(scaled, -code_limit, code_limit).astype(jnp.bfloat16)

    loads[1].wait()
    encode(0, part)

    if mates:
        greeted_more = any_of(
            [flag for flag, combiner in zip(in_nears, combiners) if combiner not in hubs]
        )
        greeted_more = jnp.logical_and(greeted_more, jnp.logical_not(is_idle))
        for flag, more in ((greeted_more, 1), (jnp.logical_not(greeted_more), 0)):

            @pl.when(jnp.logical_and(flag, is_hub))
            def _():
                pl.semaphore_wait(barrier, len(hubs) - 1 + more)

            @pl.when(jnp.logical_and(flag, jnp.logical_not(is_hub)))
            def _():
                pl.semaphore_wait(barrier, len(hubs) + more)

    else:

        @pl.when(is_hub)
        def _():
            pl.semaphore_wait(barrier, len(hubs) - 1)

        @unless(is_hub)
        def _():
            pl.semaphore_wait(barrier, len(hubs))

    last = fsdp - 1
    lateness = lax.div(level, max(last, 1))

    def send_part(q, where):
        @unless(at_place(where))
        def _():
            source = message.at[pl.ds(q * part, part)]
            remote(source, received.at[slot], send_sem, recv_sems.at[lateness], where).start()

    if mates:

        @pl.when(level == last)
        def _():
            source = message.at[pl.ds(0, part)]
            remote(source, received.at[slot], send_sem, recv_sems.at[lateness], mate).start()

        @unless(level == last)
        def _():
            send_part(0, proxies[0])

    else:
        send_part(0, proxies[0])
    loads[2].wait()
    encode(part, blocks - part)
    values = grads[0]

    if mates:

        @pl.when(level == last)
        def _():
            send_part(0, proxies[0])

        @unless(jnp.logical_or(is_root, is_near))
        def _():
            remote(rest, all_received.at[slot], send_sem, recv_sems.at[lateness], root).start()

        for at, combiner in enumerate(combiners):

            @pl.when(jnp.logical_and(in_nears[at], jnp.logical_not(at_place(combiner))))
            def _():
                target = near_received.at[level * pair + mine - (tops + at) * pair]
                remote(rest, target, send_sem, near_recv, combiner).start()

    drain(state, in_sems.at[3])
    if mates:

        @pl.when(is_kept)
        def _():
            target = all_states.at[me - skip // owned]
            remote(state, target, state_send, state_recv.at[lateness], root).start()

        @pl.when(jnp.logical_and(group == 0, jnp.logical_not(is_first)))
        def _():
            target = states.at[seat]
            remote(state, target, state_send, state_recv.at[lateness], mate).start()

    for q, where in enumerate(proxies):

        @pl.when(jnp.logical_and(group == q, jnp.logical_not(is_proxy)))
        def _():
            remote(state, states.at[seat], state_send, state_recv.at[lateness], where).start()

    peak_column = jnp.max(jnp.abs(values), axis=1, keepdims=True)
    peak_row = jnp.max(jnp.where(diagonal, peak_column, 0.0), axis=0, keepdims=True)
    peak_message[...] = jnp.zeros_like(peak_message)
    for line in range(lines):
        low = line * width
        high = min(low + width, blocks)
        peak_message[pl.ds(line, 1), : high - low] = peak_row[:, low:high]

    for where in mates + [collector]:

        @unless(at_place(where))
        def _():
            remote(peak_message, peak_received.at[me], peak_send, peak_recv, where).start()

    for q, where in list(enumerate(proxies))[1:]:
        send_part(q, where)

    def top_of_all():
        peak_received[me] = peak_message[...]
        drain(peak_received.at[pl.ds(0, n - 1)], peak_recv)
        return jnp.max(peak_received[...], axis=0)

    def column_of(values, first, rows):
        at_row = lax.broadcasted_iota(jnp.int32, (rows, blocks), 0)
        at_lane = lax.broadcasted_iota(jnp.int32, (rows, blocks), 1)
        return jnp.sum(jnp.where(at_lane == at_row + first, values, 0.0), axis=1, keepdims=True)

    def run_if(flag, step):
        if isinstance(flag, bool):
            if flag:
                step()
        else:
            pl.when(flag)(step)

    def negated(flag):
        return not flag if isinstance(flag, bool) else jnp.logical_not(flag)

    def place_states(target, source, owners, late):
        for at in range(owners):
            if (at % fsdp == last) == late:
                for kind in range(3):
                    target[kind, pl.ds(at * owned, owned), :] = source[at, kind]

    def summed(inbox, first, rows):
        return jnp.sum(inbox[pl.ds(first, rows)].astype(jnp.float32), axis=0)

    if mates:
        for at, (combiner, near) in enumerate(zip(combiners, nears)):

            @pl.when(at_place(combiner))
            def _():
                own = combiner in near
                if own:
                    near_received[near.index(combiner)] = message[pl.ds(skip, kept), :]
                drain(near_received.at[pl.ds(0, len(near) - own)], near_recv)
                partial_out[...] = summed(near_received, 0, len(near))
                remote(partial_out, partial_in.at[at], grad_send, top_recv, root).start()

    @pl.when(is_collector)
    def _():
        top = top_of_all()
        peak_out[...] = top

        def spread_top(where):
            remote(peak_out, peak_in, peak_send, top_recv, where).start()

        others(spread_top, mates)
        peak_in[...] = top

    if mates:

        @pl.when(is_root)
        def _():
            all_received[slot] = message[pl.ds(skip, kept), :]
            own_scale = column_of(scale, skip, kept)
            owners = kept // owned
            total = None
            direct = [tops * pair if f < near_levels else dp for f in range(fsdp)]
            drain(all_received.at[pl.ds(0, sum(direct[:last]) - 1)], recv_sems.at[0])
            for f in range(last):
                more = summed(all_received, f * dp, direct[f])
                total = more if total is None else total + more
            drain(all_states.at[pl.ds(0, (dp - pair) * last)], state_recv.at[0])
            place_states(all_column, all_states, owners, False)
            drain(partial_in, top_recv)
            total = total + summed(partial_in, 0, gathered)
            drain(all_received.at[pl.ds(0, direct[last])], recv_sems.at[1])
            total = total + summed(all_received, last * dp, direct[last])
            drain(all_states.at[pl.ds(0, dp - pair)], state_recv.at[1])
            place_states(all_column, all_states, owners, True)
            gradient = total * own_scale
            updated, _, _ = adamw(gradient, all_column[0], all_column[1], all_column[2])
            ready = weights_ref.at[pl.ds(skip, kept)]
            weights_ref[pl.ds(skip, kept), :] = updated.astype(jnp.bfloat16)
            for where in [mate] + beside:
                remote(ready, ready, out_send, out_recv, where).start()

    if mates:

        @pl.when(is_first)
        def _():
            states[pl.ds(seat, 1)] = state[...][None]
            own_scale = column_of(scale, 0, part)
            drain(states.at[pl.ds(0, pair * last - 1)], state_recv.at[0])
            place_states(column, states, pair * fsdp, False)
            drain(states.at[pl.ds(0, pair)], state_recv.at[1])
            place_states(column, states, pair * fsdp, True)
            drain(early_in, top_recv)
            drain(received.at[pl.ds(0, dp)], recv_sems.at[1])
            gradient = (early_in[...] + summed(received, last * dp, dp)) * own_scale
            codes[...] = gradient
            own = (mate[0] * fsdp + mate[1]) * owned
            gradient_in[...] = codes[pl.ds(own, owned), :]
            updated, _, _ = adamw(gradient, column[0], column[1], column[2])
            weights_ref[pl.ds(0, part), :] = updated.astype(jnp.bfloat16)

    def reduce_part(mine, level):
        group = mine // pair if isinstance(mine, int) else lax.div(mine, pair)
        seat = (mine - group * pair) * fsdp + level
        first = group * part
        if not isinstance(first, int):
            first = pl.multiple_of(first, 8)
        received[pl.ds(level * dp + mine, 1)] = message[pl.ds(first, part)][None]
        states[pl.ds(seat, 1)] = state[...][None]
        own_scale = column_of(scale, first, part)
        at_last = proxies[0][1] == last
        total = None
        for f in range(fsdp):
            if f == last:
                if mates and group == 0:
                    early_out[...] = total
                    remote(early_out, early_in, grad_send, top_recv, mate).start()
                drain(states.at[pl.ds(0, pair * last - (not at_last))], state_recv.at[0])
                place_states(column, states, pair * fsdp, False)
            if f == 0 and last:
                drain(received.at[pl.ds(0, dp * last - (not at_last))], recv_sems.at[0])
            if f == last:
                drain(received.at[pl.ds(0, dp - at_last)], recv_sems.at[min(last, 1)])
            more = summed(received, f * dp, dp)
            total = more if total is None else total + more
        drain(states.at[pl.ds(0, pair - at_last)], state_recv.at[1])
        place_states(column, states, pair * fsdp, True)
        gradient = total * own_scale
        codes[...] = gradient

        def hand_out(at):
            gradient_out[at] = codes[pl.ds(at * owned, owned), :]
            where = (group * pair + at // fsdp, at % fsdp)

            def send():
                remote(gradient_out.at[at], gradient_in, grad_send, grad_recv, where).start()

            run_if(negated(seat == at), send)

        lines_of = pl.ds(first, part)
        ready = weights_ref.at[lines_of]

        def spread(where):
            remote(ready, ready, out_send, out_recv, where).start()

        served = [root] if mates and group == 0 else []
        early = [where[0] * fsdp + where[1] for where in served]
        skipped = [mate[0] * fsdp + mate[1]] if served else []
        late = [at for at in range(pair * fsdp) if at not in early + skipped]
        for at in early if served else late:
            hand_out(at)
        updated, _, _ = adamw(gradient, column[0], column[1], column[2])
        weights_ref[lines_of, :] = updated.astype(jnp.bfloat16)
        for where in served:
            spread(where)
        for at in late if served else early:
            hand_out(at)
        if isinstance(mine, int):
            unserved = mates if group == 0 else mates + beside
            for where in [(k, f) for k in range(dp) for f in range(fsdp)]:
                if where != (mine, level) and where not in unserved:
                    spread(where)
        else:
            others(spread)
        gradient_in[...] = gradient_out[seat]

    if mates:
        for where in proxies:
            pl.when(at_place(where))(functools.partial(reduce_part, *where))
    else:
        pl.when(is_proxy)(functools.partial(reduce_part, mine, level))

    @unless(jnp.logical_or(is_proxy, is_first) if mates else is_proxy)
    def _():
        drain(gradient_in, grad_recv)

    updated, first, second = adamw(gradient_in[...], state[0], state[1], state[2])
    updated_ref[...] = updated
    first_ref[...] = first
    second_ref[...] = second

    @pl.when(is_mate)
    def _():
        peak_in[...] = top_of_all()

    @unless(any_of([is_collector, is_mate]))
    def _():
        drain(peak_in, top_recv)

    for line in range(lines):
        low = line * width
        high = min(low + width, blocks)
        peak_ref[:, low:high] = peak_in[pl.ds(line, 1), : high - low]

    def tally(flags):
        return sum(jnp.where(flag, 1, 0) for flag in flags)

    def drain_first(ref, sem, number, most):
        for value in range(1, most + 1):

            @pl.when(number == value)
            def _():
                drain(ref.at[pl.ds(0, value)], sem)

    parts_sent = count - tally([is_proxy])
    states_sent = tally([jnp.logical_not(is_proxy)])
    if mates:
        parts_sent += (count - 1) * tally([jnp.logical_not(jnp.logical_or(is_root, is_idle))])
        parts_sent += tally([level == last])
        states_sent += tally([is_kept, jnp.logical_and(group == 0, jnp.logical_not(is_first))])

        @unless(jnp.logical_or(is_proxy, is_root))
        def _():
            drain_first(received, send_sem, parts_sent, 2 * count)

        drain_first(states, state_send, states_sent, 3)

        @pl.when(any_of([at_place(where) for where in combiners]))
        def _():
            drain(partial_out, grad_send)

    else:

        @unless(is_proxy)
        def _():
            drain(message, send_sem)
            drain(state, state_send)

        @pl.when(is_proxy)
        def _():
            drain(message.at[pl.ds(0, (count - 1) * part)], send_sem)

    inboxes = len(mates) + 1
    is_inbox = any_of([is_mate, is_collector])

    @pl.when(is_collector)
    def _():
        drain(peak_received.at[pl.ds(0, n - 1)], peak_send)

    if mates:

        @pl.when(is_mate)
        def _():
            drain(peak_received.at[pl.ds(0, inboxes - 1)], peak_send)

    @unless(is_inbox)
    def _():
        drain(peak_received.at[pl.ds(0, inboxes)], peak_send)

    @pl.when(is_proxy)
    def _():
        drain(weights_ref.at[pl.ds(0, (count - 1) * part)], out_recv)

    for at, where in enumerate(proxies):

        @pl.when(at_place(where))
        def _():
            unserved = 1 if mates and at == 0 else 0
            sent = 2 * pair * fsdp - 2 if unserved else pair * fsdp - 1
            drain(gradient_out.at[pl.ds(0, sent)], grad_send)

    if mates:

        @pl.when(is_root)
        def _():
            drain(weights_ref.at[pl.ds(0, skip)], out_recv)
            drain(received.at[pl.ds(0, count + (count - 1) * (1 + len(beside)))], send_sem)

        @pl.when(is_first)
        def _():
            drain(rest, out_recv)

        @unless(any_of([is_proxy, is_mate]))
        def _():
            drain(weights_ref, out_recv)

        for at, where in enumerate(proxies):
            reached = n - 1 - (len(mates + beside) if at else 1)

            @pl.when(at_place(where))
            def _():
                sent = 2 * (count - 1) + (where[1] == last) + reached
                drain(received.at[pl.ds(0, sent)], send_sem)

    else:

        @unless(is_proxy)
        def _():
            drain(weights_ref, out_recv)

        @pl.when(is_proxy)
        def _():
            drain(received.at[pl.ds(0, n - 1)], out_send)


def finish_kernel(*refs):
    *refs, three, sems = refs
    count = len(refs) // 2
    stores = [
        pltpu.make_async_copy(refs[at], refs[count + at], sems.at[max(at - 2, 0)])
        for at in range(count)
    ]
    for store in stores:
        store.start()
    pltpu.make_async_copy(three, three, sems.at[0]).wait()
    for store in stores[3:]:
        store.wait()


def body(sizes, grads, last_peak, master, moment1, moment2):
    dp, fsdp = sizes
    n = dp * fsdp
    blocks, width = grads.shape[1:]
    pair, proxies, _, mates = layout(sizes, blocks, width)
    count = len(proxies)
    owned = master.shape[0]
    part = blocks // count
    lines = pl.cdiv(blocks, width)
    f32, bf16 = jnp.float32, jnp.bfloat16
    vmem = pl.BlockSpec(memory_space=pltpu.VMEM)
    anywhere = pl.BlockSpec(memory_space=pl.ANY)
    shapes = (
        ((owned, width), f32),
        ((owned, width), f32),
        ((owned, width), f32),
        ((blocks, width), bf16),
        ((1, blocks), f32),
    )
    kept = blocks - part
    near_levels, gathered, _ = gathering(sizes)
    root_scratch = [
        pltpu.VMEM((n, kept, width), bf16),
        pltpu.VMEM((kept // owned, 3, owned, width), f32),
        pltpu.VMEM((3, kept, width), f32),
        pltpu.VMEM((near_levels * pair, kept, width), bf16),
        pltpu.VMEM((kept, width), f32),
        pltpu.VMEM((gathered, kept, width), f32),
        pltpu.VMEM((part, width), f32),
        pltpu.VMEM((part, width), f32),
    ]
    results = pl.pallas_call(
        functools.partial(kernel, sizes),
        out_shape=tuple(pltpu.VMEM(shape, kind) for shape, kind in shapes),
        in_specs=[anywhere] * 5,
        out_specs=(vmem,) * 5,
        scratch_shapes=[
            pltpu.VMEM((1, blocks, width), f32),
            pltpu.VMEM((1, blocks), f32),
            pltpu.VMEM((3, owned, width), f32),
            pltpu.VMEM((part, width), f32),
            pltpu.VMEM((blocks, width), bf16),
            pltpu.VMEM((2 * n if mates else n, part, width), bf16),
            pltpu.VMEM((pair * fsdp, 3, owned, width), f32),
            pltpu.VMEM((3, part, width), f32),
            pltpu.VMEM((2 * pair * fsdp, owned, width), f32),
            pltpu.VMEM((owned, width), f32),
            pltpu.VMEM((lines, width), f32),
            pltpu.VMEM((n, lines, width), f32),
            pltpu.VMEM((lines, width), f32),
            pltpu.VMEM((lines, width), f32),
            pltpu.SemaphoreType.DMA((4,)),
            pltpu.SemaphoreType.DMA((2,)),
        ]
        + [pltpu.SemaphoreType.DMA] * 2
        + [pltpu.SemaphoreType.DMA((2,))]
        + [pltpu.SemaphoreType.DMA] * 6
        + (root_scratch if mates else [pltpu.SemaphoreType.DMA]),
        compiler_params=pltpu.CompilerParams(collective_id=0, has_side_effects=True),
    )(grads, last_peak.reshape(1, blocks), master, moment1, moment2)
    updated, first, second, weights, peak = pl.pallas_call(
        finish_kernel,
        out_shape=tuple(jax.ShapeDtypeStruct(shape, kind) for shape, kind in shapes),
        in_specs=[vmem] * 5,
        out_specs=(anywhere,) * 5,
        scratch_shapes=[pltpu.VMEM((3, owned, width), f32), pltpu.SemaphoreType.DMA((3,))],
    )(*(pltpu.with_memory_space_constraint(result, pltpu.VMEM) for result in results))
    return (updated, first, second, weights, peak.reshape(blocks))


def solution(mesh):
    sharded = P(AXES, None)
    return jax.shard_map(
        functools.partial(body, (mesh.shape["dp"], mesh.shape["fsdp"])),
        mesh=mesh,
        in_specs=(P(AXES, None, None), P(), sharded, sharded, sharded),
        out_specs=(sharded, sharded, sharded, P(), P()),
        check_vma=False,
    )
```

```python
import functools

import jax
import jax.numpy as jnp
from jax import lax
from jax.experimental import pallas as pl
from jax.experimental.pallas import tpu as pltpu
from jax.sharding import PartitionSpec as P

STEP_COUNT = 10


code_limit = 448.0
peak_floor = 0.05
beta_one = 0.9
beta_two = 0.95
learn_rate = 0.05
decay_rate = 0.1
epsilon = 1e-08
AXES = ("dp", "fsdp")
UNROLL_MOST = 64
ROOT_BYTES = 8 * 2**20


def adamw(gradient, master, moment1, moment2):
    first = beta_one * moment1 + (1.0 - beta_one) * gradient
    second = beta_two * moment2 + (1.0 - beta_two) * gradient * gradient
    corrected_one = first * (1.0 / (1.0 - beta_one**STEP_COUNT))
    corrected_two = second * (1.0 / (1.0 - beta_two**STEP_COUNT))
    updated = master - learn_rate * (
        corrected_one / (jnp.sqrt(corrected_two) + epsilon) + decay_rate * master
    )
    return (updated, first, second)


def layout(sizes, blocks, width):
    dp, fsdp = sizes
    pair = 2 if dp % 2 == 0 else 1
    above = min(1, fsdp - 1)
    proxies = [(pair * q + pair - 1, above) for q in range(dp // pair)]
    collector = (min(3, dp - 1), 0)
    mates = [(k, 0) for k in range(pair)]
    fits = 2 * dp * fsdp * blocks * width <= ROOT_BYTES
    if above == 0 or pair == 1 or dp < 4 * pair or dp % (2 * pair) or not fits:
        mates = []
    return pair, proxies, collector, mates


def gathering(sizes):
    dp, fsdp = sizes
    chips = dp // 2
    count = chips // 4
    return min(2, fsdp - 1), count, [(2 * (g - chips // 2) + 1, 0) for g in range(chips - count, chips)]


def near_root(sizes):
    dp, fsdp = sizes
    return [(3, 0), (dp // 2 + 1, 0)] + [(1, f) for f in range(1, fsdp - 1)]


def kernel(
    sizes,
    grads_hbm,
    last_peak_hbm,
    master_hbm,
    moment1_hbm,
    moment2_hbm,
    updated_ref,
    first_ref,
    second_ref,
    weights_ref,
    peak_ref,
    grads,
    last_peak,
    state,
    codes,
    message,
    received,
    states,
    column,
    gradient_out,
    gradient_in,
    peak_message,
    peak_received,
    peak_out,
    peak_in,
    in_sems,
    recv_sems,
    send_sem,
    state_send,
    state_recv,
    grad_send,
    grad_recv,
    out_recv,
    peak_send,
    peak_recv,
    top_recv,
    *root_refs,
):
    dp, fsdp = sizes
    n = dp * fsdp
    blocks, width = message.shape
    pair, proxies, collector, mates = layout(sizes, blocks, width)
    count = len(proxies)
    hubs = proxies + [collector] + mates
    owned = blocks // n
    part = blocks // count
    lines = peak_out.shape[0]
    mine, level = lax.axis_index("dp"), lax.axis_index("fsdp")
    me = mine * fsdp + level
    slot = level * dp + mine
    group = lax.div(mine, pair)
    seat = lax.rem(mine, pair) * fsdp + level

    def at_place(where):
        return jnp.logical_and(mine == where[0], level == where[1])

    def any_of(flags):
        return functools.reduce(jnp.logical_or, flags, jnp.bool_(False))

    def unless(flag):
        return pl.when(jnp.logical_not(flag))

    is_proxy = any_of([at_place(where) for where in proxies])
    is_collector = at_place(collector)
    is_mate = any_of([at_place(where) for where in mates])
    is_hub = any_of([is_proxy, is_collector, is_mate])
    if mates:
        root = mates[-1]
        is_root = at_place(root)
        skip, kept = part, blocks - part
        rest = message.at[pl.ds(skip, kept)]
        is_kept = me * owned >= skip
        mate = mates[0]
        beside = near_root(sizes)
        is_first = at_place(mate)
        near_levels, gathered, combiners = gathering(sizes)
        tops = dp // pair - gathered
        nears = []
        for at in range(gathered):
            chip = (tops + at) * pair
            nears.append([(k, f) for f in range(near_levels) for k in range(chip, chip + pair)])
        in_nears = [jnp.logical_and(level < near_levels, group == tops + at) for at in range(gathered)]
        is_near = any_of(in_nears)
        idle = [where for where, near in zip(combiners, nears) if where in near]
        is_idle = any_of([at_place(where) for where in idle])
        (
            all_received,
            all_states,
            all_column,
            near_received,
            partial_out,
            partial_in,
            early_out,
            early_in,
        ) = root_refs
        out_send = send_sem
        near_recv = recv_sems.at[0]
    else:
        (out_send,) = root_refs

    def remote(source, target, send, recv, where):
        return pltpu.make_async_remote_copy(
            src_ref=source,
            dst_ref=target,
            send_sem=send,
            recv_sem=recv,
            device_id=where,
            device_id_type=pl.DeviceIdType.MESH,
        )

    def drain(ref, sem):
        pltpu.make_async_copy(ref, ref, sem).wait()

    def others(step, skipped=()):
        if n <= UNROLL_MOST:
            near = [(k, f) for f in range(fsdp) for k in range(pair)]
            far = [(k, f) for f in range(fsdp) for k in range(pair, dp)]
            for where in near + far:
                if where not in skipped:
                    unless(at_place(where))(functools.partial(step, where))
        else:

            def turn(k, carry):
                other = lax.rem(me + k, n)
                step((lax.div(other, fsdp), lax.rem(other, fsdp)))
                return carry

            lax.fori_loop(1, n, turn, 0)

    loads = [
        pltpu.make_async_copy(source, target, in_sems.at[min(at, 3)])
        for at, (source, target) in enumerate(
            (
                (last_peak_hbm, last_peak),
                (grads_hbm.at[:, pl.ds(0, part)], grads.at[:, pl.ds(0, part)]),
                (grads_hbm.at[:, pl.ds(part, blocks - part)], grads.at[:, pl.ds(part, blocks - part)]),
                (master_hbm, state.at[0]),
                (moment1_hbm, state.at[1]),
                (moment2_hbm, state.at[2]),
            )
        )
    ]
    for load in loads:
        load.start()
    barrier = pltpu.get_barrier_semaphore()

    def greet(where):
        pl.semaphore_signal(
            barrier, inc=1, device_id=where, device_id_type=pl.DeviceIdType.MESH
        )

    @pl.when(is_hub)
    def _():
        others(greet)

    if mates:

        for combiner, near in zip(combiners, nears):
            if combiner not in hubs:

                @pl.when(at_place(combiner))
                def _():
                    for where in near:
                        if where != combiner:
                            greet(where)

    loads[0].wait()
    floored = jnp.maximum(last_peak[...], peak_floor)
    inverse = code_limit / floored
    scale = floored / code_limit
    row = lax.broadcasted_iota(jnp.int32, (blocks, blocks), 0)
    lane = lax.broadcasted_iota(jnp.int32, (blocks, blocks), 1)
    diagonal = row == lane
    inverse_column = jnp.sum(jnp.where(diagonal, inverse, 0.0), axis=1, keepdims=True)
    def encode(first, rows):
        scaled = grads[0, pl.ds(first, rows), :] * inverse_column[first : first + rows]
        message[pl.ds(first, rows), :] = jnp.clip(scaled, -code_limit, code_limit).astype(jnp.bfloat16)

    loads[1].wait()
    encode(0, part)

    if mates:
        greeted_more = any_of(
            [flag for flag, combiner in zip(in_nears, combiners) if combiner not in hubs]
        )
        greeted_more = jnp.logical_and(greeted_more, jnp.logical_not(is_idle))
        for flag, more in ((greeted_more, 1), (jnp.logical_not(greeted_more), 0)):

            @pl.when(jnp.logical_and(flag, is_hub))
            def _():
                pl.semaphore_wait(barrier, len(hubs) - 1 + more)

            @pl.when(jnp.logical_and(flag, jnp.logical_not(is_hub)))
            def _():
                pl.semaphore_wait(barrier, len(hubs) + more)

    else:

        @pl.when(is_hub)
        def _():
            pl.semaphore_wait(barrier, len(hubs) - 1)

        @unless(is_hub)
        def _():
            pl.semaphore_wait(barrier, len(hubs))

    last = fsdp - 1
    lateness = lax.div(level, max(last, 1))

    def send_part(q, where):
        @unless(at_place(where))
        def _():
            source = message.at[pl.ds(q * part, part)]
            remote(source, received.at[slot], send_sem, recv_sems.at[lateness], where).start()

    if mates:

        @pl.when(level == last)
        def _():
            source = message.at[pl.ds(0, part)]
            remote(source, received.at[slot], send_sem, recv_sems.at[lateness], mate).start()
            send_part(0, proxies[0])

        @unless(level == last)
        def _():
            send_part(0, proxies[0])

    else:
        send_part(0, proxies[0])
    loads[2].wait()
    encode(part, blocks - part)
    values = grads[0]

    if mates:

        @unless(jnp.logical_or(is_root, is_near))
        def _():
            remote(rest, all_received.at[slot], send_sem, recv_sems.at[lateness], root).start()

        for at, combiner in enumerate(combiners):

            @pl.when(jnp.logical_and(in_nears[at], jnp.logical_not(at_place(combiner))))
            def _():
                target = near_received.at[level * pair + mine - (tops + at) * pair]
                remote(rest, target, send_sem, near_recv, combiner).start()

    drain(state, in_sems.at[3])
    if mates:

        @pl.when(is_kept)
        def _():
            target = all_states.at[me - skip // owned]
            remote(state, target, state_send, state_recv.at[lateness], root).start()

        @pl.when(jnp.logical_and(group == 0, jnp.logical_not(is_first)))
        def _():
            target = states.at[seat]
            remote(state, target, state_send, state_recv.at[lateness], mate).start()

    for q, where in enumerate(proxies):

        @pl.when(jnp.logical_and(group == q, jnp.logical_not(is_proxy)))
        def _():
            remote(state, states.at[seat], state_send, state_recv.at[lateness], where).start()

    peak_column = jnp.max(jnp.abs(values), axis=1, keepdims=True)
    peak_row = jnp.max(jnp.where(diagonal, peak_column, 0.0), axis=0, keepdims=True)
    peak_message[...] = jnp.zeros_like(peak_message)
    for line in range(lines):
        low = line * width
        high = min(low + width, blocks)
        peak_message[pl.ds(line, 1), : high - low] = peak_row[:, low:high]

    for where in mates + [collector]:

        @unless(at_place(where))
        def _():
            remote(peak_message, peak_received.at[me], peak_send, peak_recv, where).start()

    for q, where in list(enumerate(proxies))[1:]:
        send_part(q, where)

    def top_of_all():
        peak_received[me] = peak_message[...]
        drain(peak_received.at[pl.ds(0, n - 1)], peak_recv)
        return jnp.max(peak_received[...], axis=0)

    def column_of(values, first, rows):
        at_row = lax.broadcasted_iota(jnp.int32, (rows, blocks), 0)
        at_lane = lax.broadcasted_iota(jnp.int32, (rows, blocks), 1)
        return jnp.sum(jnp.where(at_lane == at_row + first, values, 0.0), axis=1, keepdims=True)

    def run_if(flag, step):
        if isinstance(flag, bool):
            if flag:
                step()
        else:
            pl.when(flag)(step)

    def negated(flag):
        return not flag if isinstance(flag, bool) else jnp.logical_not(flag)

    def place_states(target, source, owners, late):
        for at in range(owners):
            if (at % fsdp == last) == late:
                for kind in range(3):
                    target[kind, pl.ds(at * owned, owned), :] = source[at, kind]

    def summed(inbox, first, rows):
        return jnp.sum(inbox[pl.ds(first, rows)].astype(jnp.float32), axis=0)

    if mates:
        for at, (combiner, near) in enumerate(zip(combiners, nears)):

            @pl.when(at_place(combiner))
            def _():
                own = combiner in near
                if own:
                    near_received[near.index(combiner)] = message[pl.ds(skip, kept), :]
                drain(near_received.at[pl.ds(0, len(near) - own)], near_recv)
                partial_out[...] = summed(near_received, 0, len(near))
                remote(partial_out, partial_in.at[at], grad_send, top_recv, root).start()

    @pl.when(is_collector)
    def _():
        top = top_of_all()
        peak_out[...] = top

        def spread_top(where):
            remote(peak_out, peak_in, peak_send, top_recv, where).start()

        others(spread_top, mates)
        peak_in[...] = top

    if mates:

        @pl.when(is_root)
        def _():
            all_received[slot] = message[pl.ds(skip, kept), :]
            own_scale = column_of(scale, skip, kept)
            owners = kept // owned
            total = None
            direct = [tops * pair if f < near_levels else dp for f in range(fsdp)]
            drain(all_received.at[pl.ds(0, sum(direct[:last]) - 1)], recv_sems.at[0])
            for f in range(last):
                more = summed(all_received, f * dp, direct[f])
                total = more if total is None else total + more
            drain(all_states.at[pl.ds(0, (dp - pair) * last)], state_recv.at[0])
            place_states(all_column, all_states, owners, False)
            drain(partial_in, top_recv)
            total = total + summed(partial_in, 0, gathered)
            drain(all_received.at[pl.ds(0, direct[last])], recv_sems.at[1])
            total = total + summed(all_received, last * dp, direct[last])
            drain(all_states.at[pl.ds(0, dp - pair)], state_recv.at[1])
            place_states(all_column, all_states, owners, True)
            gradient = total * own_scale
            updated, _, _ = adamw(gradient, all_column[0], all_column[1], all_column[2])
            ready = weights_ref.at[pl.ds(skip, kept)]
            weights_ref[pl.ds(skip, kept), :] = updated.astype(jnp.bfloat16)
            for where in [mate] + beside:
                remote(ready, ready, out_send, out_recv, where).start()

    if mates:

        @pl.when(is_first)
        def _():
            states[pl.ds(seat, 1)] = state[...][None]
            own_scale = column_of(scale, 0, part)
            drain(states.at[pl.ds(0, pair * last - 1)], state_recv.at[0])
            place_states(column, states, pair * fsdp, False)
            drain(states.at[pl.ds(0, pair)], state_recv.at[1])
            place_states(column, states, pair * fsdp, True)
            drain(early_in, top_recv)
            drain(received.at[pl.ds(0, dp)], recv_sems.at[1])
            gradient = (early_in[...] + summed(received, last * dp, dp)) * own_scale
            codes[...] = gradient
            own = (mate[0] * fsdp + mate[1]) * owned
            gradient_in[...] = codes[pl.ds(own, owned), :]
            updated, _, _ = adamw(gradient, column[0], column[1], column[2])
            weights_ref[pl.ds(0, part), :] = updated.astype(jnp.bfloat16)

    def reduce_part(mine, level):
        group = mine // pair if isinstance(mine, int) else lax.div(mine, pair)
        seat = (mine - group * pair) * fsdp + level
        first = group * part
        if not isinstance(first, int):
            first = pl.multiple_of(first, 8)
        received[pl.ds(level * dp + mine, 1)] = message[pl.ds(first, part)][None]
        states[pl.ds(seat, 1)] = state[...][None]
        own_scale = column_of(scale, first, part)
        at_last = proxies[0][1] == last
        total = None
        for f in range(fsdp):
            if f == last:
                if mates and group == 0:
                    early_out[...] = total
                    remote(early_out, early_in, grad_send, top_recv, mate).start()
                drain(states.at[pl.ds(0, pair * last - (not at_last))], state_recv.at[0])
                place_states(column, states, pair * fsdp, False)
            if f == 0 and last:
                drain(received.at[pl.ds(0, dp * last - (not at_last))], recv_sems.at[0])
            if f == last:
                drain(received.at[pl.ds(0, dp - at_last)], recv_sems.at[min(last, 1)])
            more = summed(received, f * dp, dp)
            total = more if total is None else total + more
        drain(states.at[pl.ds(0, pair - at_last)], state_recv.at[1])
        place_states(column, states, pair * fsdp, True)
        gradient = total * own_scale
        codes[...] = gradient

        def hand_out(at):
            gradient_out[at] = codes[pl.ds(at * owned, owned), :]
            where = (group * pair + at // fsdp, at % fsdp)

            def send():
                remote(gradient_out.at[at], gradient_in, grad_send, grad_recv, where).start()

            run_if(negated(seat == at), send)

        lines_of = pl.ds(first, part)
        ready = weights_ref.at[lines_of]

        def spread(where):
            remote(ready, ready, out_send, out_recv, where).start()

        served = [root] if mates and group == 0 else []
        early = [where[0] * fsdp + where[1] for where in served]
        skipped = [mate[0] * fsdp + mate[1]] if served else []
        late = [at for at in range(pair * fsdp) if at not in early + skipped]
        for at in early if served else late:
            hand_out(at)
        updated, _, _ = adamw(gradient, column[0], column[1], column[2])
        weights_ref[lines_of, :] = updated.astype(jnp.bfloat16)
        for where in served:
            spread(where)
        for at in late if served else early:
            hand_out(at)
        if isinstance(mine, int):
            unserved = mates if group == 0 else mates + beside
            for where in [(k, f) for k in range(dp) for f in range(fsdp)]:
                if where != (mine, level) and where not in unserved:
                    spread(where)
        else:
            others(spread)
        gradient_in[...] = gradient_out[seat]

    if mates:
        for where in proxies:
            pl.when(at_place(where))(functools.partial(reduce_part, *where))
    else:
        pl.when(is_proxy)(functools.partial(reduce_part, mine, level))

    @unless(jnp.logical_or(is_proxy, is_first) if mates else is_proxy)
    def _():
        drain(gradient_in, grad_recv)

    updated, first, second = adamw(gradient_in[...], state[0], state[1], state[2])
    updated_ref[...] = updated
    first_ref[...] = first
    second_ref[...] = second

    @pl.when(is_mate)
    def _():
        peak_in[...] = top_of_all()

    @unless(any_of([is_collector, is_mate]))
    def _():
        drain(peak_in, top_recv)

    for line in range(lines):
        low = line * width
        high = min(low + width, blocks)
        peak_ref[:, low:high] = peak_in[pl.ds(line, 1), : high - low]

    def tally(flags):
        return sum(jnp.where(flag, 1, 0) for flag in flags)

    def drain_first(ref, sem, number, most):
        for value in range(1, most + 1):

            @pl.when(number == value)
            def _():
                drain(ref.at[pl.ds(0, value)], sem)

    parts_sent = count - tally([is_proxy])
    states_sent = tally([jnp.logical_not(is_proxy)])
    if mates:
        parts_sent += (count - 1) * tally([jnp.logical_not(jnp.logical_or(is_root, is_idle))])
        parts_sent += tally([level == last])
        states_sent += tally([is_kept, jnp.logical_and(group == 0, jnp.logical_not(is_first))])

        @unless(jnp.logical_or(is_proxy, is_root))
        def _():
            drain_first(received, send_sem, parts_sent, 2 * count)

        drain_first(states, state_send, states_sent, 3)

        @pl.when(any_of([at_place(where) for where in combiners]))
        def _():
            drain(partial_out, grad_send)

    else:

        @unless(is_proxy)
        def _():
            drain(message, send_sem)
            drain(state, state_send)

        @pl.when(is_proxy)
        def _():
            drain(message.at[pl.ds(0, (count - 1) * part)], send_sem)

    inboxes = len(mates) + 1
    is_inbox = any_of([is_mate, is_collector])

    @pl.when(is_collector)
    def _():
        drain(peak_received.at[pl.ds(0, n - 1)], peak_send)

    if mates:

        @pl.when(is_mate)
        def _():
            drain(peak_received.at[pl.ds(0, inboxes - 1)], peak_send)

    @unless(is_inbox)
    def _():
        drain(peak_received.at[pl.ds(0, inboxes)], peak_send)

    @pl.when(is_proxy)
    def _():
        drain(weights_ref.at[pl.ds(0, (count - 1) * part)], out_recv)

    for at, where in enumerate(proxies):

        @pl.when(at_place(where))
        def _():
            unserved = 1 if mates and at == 0 else 0
            sent = 2 * pair * fsdp - 2 if unserved else pair * fsdp - 1
            drain(gradient_out.at[pl.ds(0, sent)], grad_send)

    if mates:

        @pl.when(is_root)
        def _():
            drain(weights_ref.at[pl.ds(0, skip)], out_recv)
            drain(received.at[pl.ds(0, count + (count - 1) * (1 + len(beside)))], send_sem)

        @pl.when(is_first)
        def _():
            drain(rest, out_recv)

        @unless(any_of([is_proxy, is_mate]))
        def _():
            drain(weights_ref, out_recv)

        for at, where in enumerate(proxies):
            reached = n - 1 - (len(mates + beside) if at else 1)

            @pl.when(at_place(where))
            def _():
                sent = 2 * (count - 1) + (where[1] == last) + reached
                drain(received.at[pl.ds(0, sent)], send_sem)

    else:

        @unless(is_proxy)
        def _():
            drain(weights_ref, out_recv)

        @pl.when(is_proxy)
        def _():
            drain(received.at[pl.ds(0, n - 1)], out_send)


def finish_kernel(*refs):
    *refs, shape, sems = refs
    count = len(refs) // 2
    stores = [
        pltpu.make_async_copy(refs[at], refs[count + at], sems.at[max(at - 3, 0)])
        for at in range(count)
    ]
    for store in stores:
        store.start()
    pltpu.make_async_copy(shape, shape, sems.at[0]).wait()
    for store in stores[4:]:
        store.wait()


def body(sizes, grads, last_peak, master, moment1, moment2):
    dp, fsdp = sizes
    n = dp * fsdp
    blocks, width = grads.shape[1:]
    pair, proxies, _, mates = layout(sizes, blocks, width)
    count = len(proxies)
    owned = master.shape[0]
    part = blocks // count
    lines = pl.cdiv(blocks, width)
    f32, bf16 = jnp.float32, jnp.bfloat16
    vmem = pl.BlockSpec(memory_space=pltpu.VMEM)
    anywhere = pl.BlockSpec(memory_space=pl.ANY)
    shapes = (
        ((owned, width), f32),
        ((owned, width), f32),
        ((owned, width), f32),
        ((blocks, width), bf16),
        ((1, blocks), f32),
    )
    kept = blocks - part
    near_levels, gathered, _ = gathering(sizes)
    root_scratch = [
        pltpu.VMEM((n, kept, width), bf16),
        pltpu.VMEM((kept // owned, 3, owned, width), f32),
        pltpu.VMEM((3, kept, width), f32),
        pltpu.VMEM((near_levels * pair, kept, width), bf16),
        pltpu.VMEM((kept, width), f32),
        pltpu.VMEM((gathered, kept, width), f32),
        pltpu.VMEM((part, width), f32),
        pltpu.VMEM((part, width), f32),
    ]
    results = pl.pallas_call(
        functools.partial(kernel, sizes),
        out_shape=tuple(pltpu.VMEM(shape, kind) for shape, kind in shapes),
        in_specs=[anywhere] * 5,
        out_specs=(vmem,) * 5,
        scratch_shapes=[
            pltpu.VMEM((1, blocks, width), f32),
            pltpu.VMEM((1, blocks), f32),
            pltpu.VMEM((3, owned, width), f32),
            pltpu.VMEM((part, width), f32),
            pltpu.VMEM((blocks, width), bf16),
            pltpu.VMEM((2 * n if mates else n, part, width), bf16),
            pltpu.VMEM((pair * fsdp, 3, owned, width), f32),
            pltpu.VMEM((3, part, width), f32),
            pltpu.VMEM((2 * pair * fsdp, owned, width), f32),
            pltpu.VMEM((owned, width), f32),
            pltpu.VMEM((lines, width), f32),
            pltpu.VMEM((n, lines, width), f32),
            pltpu.VMEM((lines, width), f32),
            pltpu.VMEM((lines, width), f32),
            pltpu.SemaphoreType.DMA((4,)),
            pltpu.SemaphoreType.DMA((2,)),
        ]
        + [pltpu.SemaphoreType.DMA] * 2
        + [pltpu.SemaphoreType.DMA((2,))]
        + [pltpu.SemaphoreType.DMA] * 6
        + (root_scratch if mates else [pltpu.SemaphoreType.DMA]),
        compiler_params=pltpu.CompilerParams(collective_id=0, has_side_effects=True),
    )(grads, last_peak.reshape(1, blocks), master, moment1, moment2)
    updated, first, second, weights, peak = pl.pallas_call(
        finish_kernel,
        out_shape=tuple(jax.ShapeDtypeStruct(shape, kind) for shape, kind in shapes),
        in_specs=[vmem] * 5,
        out_specs=(anywhere,) * 5,
        scratch_shapes=[pltpu.VMEM((3 + dp * fsdp // 2, owned, width), f32), pltpu.SemaphoreType.DMA((2,))],
    )(*(pltpu.with_memory_space_constraint(result, pltpu.VMEM) for result in results))
    return (updated, first, second, weights, peak.reshape(blocks))


def solution(mesh):
    sharded = P(AXES, None)
    return jax.shard_map(
        functools.partial(body, (mesh.shape["dp"], mesh.shape["fsdp"])),
        mesh=mesh,
        in_specs=(P(AXES, None, None), P(), sharded, sharded, sharded),
        out_specs=(sharded, sharded, sharded, P(), P()),
        check_vma=False,
    )
```

```python
import functools

import jax
import jax.numpy as jnp
from jax import lax
from jax.experimental import pallas as pl
from jax.experimental.pallas import tpu as pltpu
from jax.sharding import PartitionSpec as P

STEP_COUNT = 10


code_limit = 448.0
peak_floor = 0.05
beta_one = 0.9
beta_two = 0.95
learn_rate = 0.05
decay_rate = 0.1
epsilon = 1e-08
AXES = ("dp", "fsdp")
UNROLL_MOST = 64
ROOT_BYTES = 8 * 2**20


def adamw(gradient, master, moment1, moment2):
    first = beta_one * moment1 + (1.0 - beta_one) * gradient
    second = beta_two * moment2 + (1.0 - beta_two) * gradient * gradient
    corrected_one = first * (1.0 / (1.0 - beta_one**STEP_COUNT))
    corrected_two = second * (1.0 / (1.0 - beta_two**STEP_COUNT))
    updated = master - learn_rate * (
        corrected_one / (jnp.sqrt(corrected_two) + epsilon) + decay_rate * master
    )
    return (updated, first, second)


def layout(sizes, blocks, width):
    dp, fsdp = sizes
    pair = 2 if dp % 2 == 0 else 1
    above = min(1, fsdp - 1)
    proxies = [(pair * q + pair - 1, above) for q in range(dp // pair)]
    collector = (min(3, dp - 1), 0)
    mates = [(k, 0) for k in range(pair)]
    fits = 2 * dp * fsdp * blocks * width <= ROOT_BYTES
    if above == 0 or pair == 1 or dp < 4 * pair or dp % (2 * pair) or not fits:
        mates = []
    return pair, proxies, collector, mates


def gathering(sizes):
    dp, fsdp = sizes
    chips = dp // 2
    count = chips // 4
    return min(2, fsdp - 1), count, [(2 * (g - chips // 2) + 1, 0) for g in range(chips - count, chips)]


def near_root(sizes):
    dp, fsdp = sizes
    return [(3, 0), (dp // 2 + 1, 0)] + [(1, f) for f in range(1, fsdp - 1)]


def kernel(
    sizes,
    grads_hbm,
    last_peak_hbm,
    master_hbm,
    moment1_hbm,
    moment2_hbm,
    updated_ref,
    first_ref,
    second_ref,
    weights_ref,
    peak_ref,
    grads,
    last_peak,
    state,
    codes,
    message,
    received,
    states,
    column,
    gradient_out,
    gradient_in,
    peak_message,
    peak_received,
    peak_out,
    peak_in,
    in_sems,
    recv_sems,
    send_sem,
    state_send,
    state_recv,
    grad_send,
    grad_recv,
    out_recv,
    peak_send,
    peak_recv,
    top_recv,
    *root_refs,
):
    dp, fsdp = sizes
    n = dp * fsdp
    blocks, width = message.shape
    pair, proxies, collector, mates = layout(sizes, blocks, width)
    count = len(proxies)
    hubs = proxies + [collector] + mates
    owned = blocks // n
    part = blocks // count
    lines = peak_out.shape[0]
    mine, level = lax.axis_index("dp"), lax.axis_index("fsdp")
    me = mine * fsdp + level
    slot = level * dp + mine
    group = lax.div(mine, pair)
    seat = lax.rem(mine, pair) * fsdp + level

    def at_place(where):
        return jnp.logical_and(mine == where[0], level == where[1])

    def any_of(flags):
        return functools.reduce(jnp.logical_or, flags, jnp.bool_(False))

    def unless(flag):
        return pl.when(jnp.logical_not(flag))

    is_proxy = any_of([at_place(where) for where in proxies])
    is_collector = at_place(collector)
    is_mate = any_of([at_place(where) for where in mates])
    is_hub = any_of([is_proxy, is_collector, is_mate])
    if mates:
        root = mates[-1]
        is_root = at_place(root)
        skip, kept = part, blocks - part
        rest = message.at[pl.ds(skip, kept)]
        is_kept = me * owned >= skip
        mate = mates[0]
        beside = near_root(sizes)
        is_first = at_place(mate)
        near_levels, gathered, combiners = gathering(sizes)
        tops = dp // pair - gathered
        nears = []
        for at in range(gathered):
            chip = (tops + at) * pair
            nears.append([(k, f) for f in range(near_levels) for k in range(chip, chip + pair)])
        in_nears = [jnp.logical_and(level < near_levels, group == tops + at) for at in range(gathered)]
        is_near = any_of(in_nears)
        idle = [where for where, near in zip(combiners, nears) if where in near]
        is_idle = any_of([at_place(where) for where in idle])
        (
            all_received,
            all_states,
            all_column,
            near_received,
            partial_out,
            partial_in,
            early_out,
            early_in,
        ) = root_refs
        out_send = send_sem
        near_recv = recv_sems.at[0]
    else:
        (out_send,) = root_refs

    def remote(source, target, send, recv, where):
        return pltpu.make_async_remote_copy(
            src_ref=source,
            dst_ref=target,
            send_sem=send,
            recv_sem=recv,
            device_id=where,
            device_id_type=pl.DeviceIdType.MESH,
        )

    def drain(ref, sem):
        pltpu.make_async_copy(ref, ref, sem).wait()

    def others(step, skipped=()):
        if n <= UNROLL_MOST:
            near = [(k, f) for f in range(fsdp) for k in range(pair)]
            far = [(k, f) for f in range(fsdp) for k in range(pair, dp)]
            for where in near + far:
                if where not in skipped:
                    unless(at_place(where))(functools.partial(step, where))
        else:

            def turn(k, carry):
                other = lax.rem(me + k, n)
                step((lax.div(other, fsdp), lax.rem(other, fsdp)))
                return carry

            lax.fori_loop(1, n, turn, 0)

    loads = [
        pltpu.make_async_copy(source, target, in_sems.at[min(at, 3)])
        for at, (source, target) in enumerate(
            (
                (last_peak_hbm, last_peak),
                (grads_hbm.at[:, pl.ds(0, part)], grads.at[:, pl.ds(0, part)]),
                (grads_hbm.at[:, pl.ds(part, blocks - part)], grads.at[:, pl.ds(part, blocks - part)]),
                (master_hbm, state.at[0]),
                (moment1_hbm, state.at[1]),
                (moment2_hbm, state.at[2]),
            )
        )
    ]
    for load in loads:
        load.start()
    barrier = pltpu.get_barrier_semaphore()

    def greet(where):
        pl.semaphore_signal(
            barrier, inc=1, device_id=where, device_id_type=pl.DeviceIdType.MESH
        )

    @pl.when(is_hub)
    def _():
        others(greet)

    if mates:

        for combiner, near in zip(combiners, nears):
            if combiner not in hubs:

                @pl.when(at_place(combiner))
                def _():
                    for where in near:
                        if where != combiner:
                            greet(where)

    loads[0].wait()
    floored = jnp.maximum(last_peak[...], peak_floor)
    inverse = code_limit / floored
    scale = floored / code_limit
    row = lax.broadcasted_iota(jnp.int32, (blocks, blocks), 0)
    lane = lax.broadcasted_iota(jnp.int32, (blocks, blocks), 1)
    diagonal = row == lane
    inverse_column = jnp.sum(jnp.where(diagonal, inverse, 0.0), axis=1, keepdims=True)
    def encode(first, rows):
        scaled = grads[0, pl.ds(first, rows), :] * inverse_column[first : first + rows]
        message[pl.ds(first, rows), :] = jnp.clip(scaled, -code_limit, code_limit).astype(jnp.bfloat16)

    loads[1].wait()
    encode(0, part)

    if mates:
        greeted_more = any_of(
            [flag for flag, combiner in zip(in_nears, combiners) if combiner not in hubs]
        )
        greeted_more = jnp.logical_and(greeted_more, jnp.logical_not(is_idle))
        for flag, more in ((greeted_more, 1), (jnp.logical_not(greeted_more), 0)):

            @pl.when(jnp.logical_and(flag, is_hub))
            def _():
                pl.semaphore_wait(barrier, len(hubs) - 1 + more)

            @pl.when(jnp.logical_and(flag, jnp.logical_not(is_hub)))
            def _():
                pl.semaphore_wait(barrier, len(hubs) + more)

    else:

        @pl.when(is_hub)
        def _():
            pl.semaphore_wait(barrier, len(hubs) - 1)

        @unless(is_hub)
        def _():
            pl.semaphore_wait(barrier, len(hubs))

    last = fsdp - 1
    lateness = lax.div(level, max(last, 1))

    def send_part(q, where):
        @unless(at_place(where))
        def _():
            source = message.at[pl.ds(q * part, part)]
            remote(source, received.at[slot], send_sem, recv_sems.at[lateness], where).start()

    if mates:

        @pl.when(level == last)
        def _():
            source = message.at[pl.ds(0, part)]
            remote(source, received.at[slot], send_sem, recv_sems.at[lateness], mate).start()
            send_part(0, proxies[0])

        @unless(level == last)
        def _():
            send_part(0, proxies[0])

    else:
        send_part(0, proxies[0])
    loads[2].wait()
    encode(part, blocks - part)
    values = grads[0]

    if mates:

        @unless(jnp.logical_or(is_root, is_near))
        def _():
            remote(rest, all_received.at[slot], send_sem, recv_sems.at[lateness], root).start()

        for at, combiner in enumerate(combiners):

            @pl.when(jnp.logical_and(in_nears[at], jnp.logical_not(at_place(combiner))))
            def _():
                target = near_received.at[level * pair + mine - (tops + at) * pair]
                remote(rest, target, send_sem, near_recv, combiner).start()

    drain(state, in_sems.at[3])
    if mates:

        @pl.when(is_kept)
        def _():
            target = all_states.at[me - skip // owned]
            remote(state, target, state_send, state_recv.at[lateness], root).start()

        @pl.when(jnp.logical_and(group == 0, jnp.logical_not(is_first)))
        def _():
            target = states.at[seat]
            remote(state, target, state_send, state_recv.at[lateness], mate).start()

    for q, where in enumerate(proxies):

        @pl.when(jnp.logical_and(group == q, jnp.logical_not(is_proxy)))
        def _():
            remote(state, states.at[seat], state_send, state_recv.at[lateness], where).start()

    peak_column = jnp.max(jnp.abs(values), axis=1, keepdims=True)
    peak_row = jnp.max(jnp.where(diagonal, peak_column, 0.0), axis=0, keepdims=True)
    peak_message[...] = jnp.zeros_like(peak_message)
    for line in range(lines):
        low = line * width
        high = min(low + width, blocks)
        peak_message[pl.ds(line, 1), : high - low] = peak_row[:, low:high]

    for where in mates + [collector]:

        @unless(at_place(where))
        def _():
            remote(peak_message, peak_received.at[me], peak_send, peak_recv, where).start()

    for q, where in list(enumerate(proxies))[1:]:
        send_part(q, where)

    def top_of_all():
        peak_received[me] = peak_message[...]
        drain(peak_received.at[pl.ds(0, n - 1)], peak_recv)
        return jnp.max(peak_received[...], axis=0)

    def column_of(values, first, rows):
        at_row = lax.broadcasted_iota(jnp.int32, (rows, blocks), 0)
        at_lane = lax.broadcasted_iota(jnp.int32, (rows, blocks), 1)
        return jnp.sum(jnp.where(at_lane == at_row + first, values, 0.0), axis=1, keepdims=True)

    def run_if(flag, step):
        if isinstance(flag, bool):
            if flag:
                step()
        else:
            pl.when(flag)(step)

    def negated(flag):
        return not flag if isinstance(flag, bool) else jnp.logical_not(flag)

    def place_states(target, source, owners, late):
        for at in range(owners):
            if (at % fsdp == last) == late:
                for kind in range(3):
                    target[kind, pl.ds(at * owned, owned), :] = source[at, kind]

    def summed(inbox, first, rows):
        return jnp.sum(inbox[pl.ds(first, rows)].astype(jnp.float32), axis=0)

    if mates:
        for at, (combiner, near) in enumerate(zip(combiners, nears)):

            @pl.when(at_place(combiner))
            def _():
                own = combiner in near
                if own:
                    near_received[near.index(combiner)] = message[pl.ds(skip, kept), :]
                drain(near_received.at[pl.ds(0, len(near) - own)], near_recv)
                partial_out[...] = summed(near_received, 0, len(near))
                remote(partial_out, partial_in.at[at], grad_send, top_recv, root).start()

    @pl.when(is_collector)
    def _():
        top = top_of_all()
        peak_out[...] = top

        def spread_top(where):
            remote(peak_out, peak_in, peak_send, top_recv, where).start()

        others(spread_top, mates)
        peak_in[...] = top

    if mates:

        @pl.when(is_root)
        def _():
            all_received[slot] = message[pl.ds(skip, kept), :]
            own_scale = column_of(scale, skip, kept)
            owners = kept // owned
            total = None
            direct = [tops * pair if f < near_levels else dp for f in range(fsdp)]
            drain(all_received.at[pl.ds(0, sum(direct[:last]) - 1)], recv_sems.at[0])
            for f in range(last):
                more = summed(all_received, f * dp, direct[f])
                total = more if total is None else total + more
            drain(all_states.at[pl.ds(0, (dp - pair) * last)], state_recv.at[0])
            place_states(all_column, all_states, owners, False)
            drain(partial_in, top_recv)
            total = total + summed(partial_in, 0, gathered)
            drain(all_received.at[pl.ds(0, direct[last])], recv_sems.at[1])
            total = total + summed(all_received, last * dp, direct[last])
            drain(all_states.at[pl.ds(0, dp - pair)], state_recv.at[1])
            place_states(all_column, all_states, owners, True)
            gradient = total * own_scale
            updated, _, _ = adamw(gradient, all_column[0], all_column[1], all_column[2])
            ready = weights_ref.at[pl.ds(skip, kept)]
            weights_ref[pl.ds(skip, kept), :] = updated.astype(jnp.bfloat16)
            for where in [mate] + beside:
                remote(ready, ready, out_send, out_recv, where).start()

    if mates:

        @pl.when(is_first)
        def _():
            states[pl.ds(seat, 1)] = state[...][None]
            own_scale = column_of(scale, 0, part)
            drain(states.at[pl.ds(0, pair * last - 1)], state_recv.at[0])
            place_states(column, states, pair * fsdp, False)
            drain(states.at[pl.ds(0, pair)], state_recv.at[1])
            place_states(column, states, pair * fsdp, True)
            drain(early_in, top_recv)
            drain(received.at[pl.ds(0, dp)], recv_sems.at[1])
            gradient = (early_in[...] + summed(received, last * dp, dp)) * own_scale
            codes[...] = gradient
            own = (mate[0] * fsdp + mate[1]) * owned
            gradient_in[...] = codes[pl.ds(own, owned), :]
            updated, _, _ = adamw(gradient, column[0], column[1], column[2])
            weights_ref[pl.ds(0, part), :] = updated.astype(jnp.bfloat16)

    def reduce_part(mine, level):
        group = mine // pair if isinstance(mine, int) else lax.div(mine, pair)
        seat = (mine - group * pair) * fsdp + level
        first = group * part
        if not isinstance(first, int):
            first = pl.multiple_of(first, 8)
        received[pl.ds(level * dp + mine, 1)] = message[pl.ds(first, part)][None]
        states[pl.ds(seat, 1)] = state[...][None]
        own_scale = column_of(scale, first, part)
        at_last = proxies[0][1] == last
        total = None
        for f in range(fsdp):
            if f == last:
                if mates and group == 0:
                    early_out[...] = total
                    remote(early_out, early_in, grad_send, top_recv, mate).start()
                drain(states.at[pl.ds(0, pair * last - (not at_last))], state_recv.at[0])
                place_states(column, states, pair * fsdp, False)
            if f == 0 and last:
                drain(received.at[pl.ds(0, dp * last - (not at_last))], recv_sems.at[0])
            if f == last:
                drain(received.at[pl.ds(0, dp - at_last)], recv_sems.at[min(last, 1)])
            more = summed(received, f * dp, dp)
            total = more if total is None else total + more
        drain(states.at[pl.ds(0, pair - at_last)], state_recv.at[1])
        place_states(column, states, pair * fsdp, True)
        gradient = total * own_scale
        codes[...] = gradient

        def hand_out(at):
            gradient_out[at] = codes[pl.ds(at * owned, owned), :]
            where = (group * pair + at // fsdp, at % fsdp)

            def send():
                remote(gradient_out.at[at], gradient_in, grad_send, grad_recv, where).start()

            run_if(negated(seat == at), send)

        lines_of = pl.ds(first, part)
        ready = weights_ref.at[lines_of]

        def spread(where):
            remote(ready, ready, out_send, out_recv, where).start()

        served = [root] if mates and group == 0 else []
        early = [where[0] * fsdp + where[1] for where in served]
        skipped = [mate[0] * fsdp + mate[1]] if served else []
        late = [at for at in range(pair * fsdp) if at not in early + skipped]
        for at in early if served else late:
            hand_out(at)
        updated, _, _ = adamw(gradient, column[0], column[1], column[2])
        weights_ref[lines_of, :] = updated.astype(jnp.bfloat16)
        for where in served:
            spread(where)
        for at in late if served else early:
            hand_out(at)
        if isinstance(mine, int):
            unserved = mates if group == 0 else mates + beside
            for where in [(k, f) for k in range(dp) for f in range(fsdp)]:
                if where != (mine, level) and where not in unserved:
                    spread(where)
        else:
            others(spread)
        gradient_in[...] = gradient_out[seat]

    if mates:
        for where in proxies:
            pl.when(at_place(where))(functools.partial(reduce_part, *where))
    else:
        pl.when(is_proxy)(functools.partial(reduce_part, mine, level))

    @unless(jnp.logical_or(is_proxy, is_first) if mates else is_proxy)
    def _():
        drain(gradient_in, grad_recv)

    updated, first, second = adamw(gradient_in[...], state[0], state[1], state[2])
    updated_ref[...] = updated
    first_ref[...] = first
    second_ref[...] = second

    @pl.when(is_mate)
    def _():
        peak_in[...] = top_of_all()

    @unless(any_of([is_collector, is_mate]))
    def _():
        drain(peak_in, top_recv)

    for line in range(lines):
        low = line * width
        high = min(low + width, blocks)
        peak_ref[:, low:high] = peak_in[pl.ds(line, 1), : high - low]

    def tally(flags):
        return sum(jnp.where(flag, 1, 0) for flag in flags)

    def drain_first(ref, sem, number, most):
        for value in range(1, most + 1):

            @pl.when(number == value)
            def _():
                drain(ref.at[pl.ds(0, value)], sem)

    parts_sent = count - tally([is_proxy])
    states_sent = tally([jnp.logical_not(is_proxy)])
    if mates:
        parts_sent += (count - 1) * tally([jnp.logical_not(jnp.logical_or(is_root, is_idle))])
        parts_sent += tally([level == last])
        states_sent += tally([is_kept, jnp.logical_and(group == 0, jnp.logical_not(is_first))])

        @unless(jnp.logical_or(is_proxy, is_root))
        def _():
            drain_first(received, send_sem, parts_sent, 2 * count)

        drain_first(states, state_send, states_sent, 3)

        @pl.when(any_of([at_place(where) for where in combiners]))
        def _():
            drain(partial_out, grad_send)

    else:

        @unless(is_proxy)
        def _():
            drain(message, send_sem)
            drain(state, state_send)

        @pl.when(is_proxy)
        def _():
            drain(message.at[pl.ds(0, (count - 1) * part)], send_sem)

    inboxes = len(mates) + 1
    is_inbox = any_of([is_mate, is_collector])

    @pl.when(is_collector)
    def _():
        drain(peak_received.at[pl.ds(0, n - 1)], peak_send)

    if mates:

        @pl.when(is_mate)
        def _():
            drain(peak_received.at[pl.ds(0, inboxes - 1)], peak_send)

    @unless(is_inbox)
    def _():
        drain(peak_received.at[pl.ds(0, inboxes)], peak_send)

    @pl.when(is_proxy)
    def _():
        drain(weights_ref.at[pl.ds(0, (count - 1) * part)], out_recv)

    for at, where in enumerate(proxies):

        @pl.when(at_place(where))
        def _():
            unserved = 1 if mates and at == 0 else 0
            sent = 2 * pair * fsdp - 2 if unserved else pair * fsdp - 1
            drain(gradient_out.at[pl.ds(0, sent)], grad_send)

    if mates:

        @pl.when(is_root)
        def _():
            drain(weights_ref.at[pl.ds(0, skip)], out_recv)
            drain(received.at[pl.ds(0, count + (count - 1) * (1 + len(beside)))], send_sem)

        @pl.when(is_first)
        def _():
            drain(rest, out_recv)

        @unless(any_of([is_proxy, is_mate]))
        def _():
            drain(weights_ref, out_recv)

        for at, where in enumerate(proxies):
            reached = n - 1 - (len(mates + beside) if at else 1)

            @pl.when(at_place(where))
            def _():
                sent = 2 * (count - 1) + (where[1] == last) + reached
                drain(received.at[pl.ds(0, sent)], send_sem)

    else:

        @unless(is_proxy)
        def _():
            drain(weights_ref, out_recv)

        @pl.when(is_proxy)
        def _():
            drain(received.at[pl.ds(0, n - 1)], out_send)


def finish_kernel(*refs):
    *refs, three, sems = refs
    count = len(refs) // 2
    stores = [
        pltpu.make_async_copy(refs[at], refs[count + at], sems.at[max(at - 2, 0)])
        for at in range(count)
    ]
    for store in stores:
        store.start()
    pltpu.make_async_copy(three, three, sems.at[0]).wait()
    for store in stores[3:]:
        store.wait()


def body(sizes, grads, last_peak, master, moment1, moment2):
    dp, fsdp = sizes
    n = dp * fsdp
    blocks, width = grads.shape[1:]
    pair, proxies, _, mates = layout(sizes, blocks, width)
    count = len(proxies)
    owned = master.shape[0]
    part = blocks // count
    lines = pl.cdiv(blocks, width)
    f32, bf16 = jnp.float32, jnp.bfloat16
    vmem = pl.BlockSpec(memory_space=pltpu.VMEM)
    anywhere = pl.BlockSpec(memory_space=pl.ANY)
    shapes = (
        ((owned, width), f32),
        ((owned, width), f32),
        ((owned, width), f32),
        ((blocks, width), bf16),
        ((1, blocks), f32),
    )
    kept = blocks - part
    near_levels, gathered, _ = gathering(sizes)
    root_scratch = [
        pltpu.VMEM((n, kept, width), bf16),
        pltpu.VMEM((kept // owned, 3, owned, width), f32),
        pltpu.VMEM((3, kept, width), f32),
        pltpu.VMEM((near_levels * pair, kept, width), bf16),
        pltpu.VMEM((kept, width), f32),
        pltpu.VMEM((gathered, kept, width), f32),
        pltpu.VMEM((part, width), f32),
        pltpu.VMEM((part, width), f32),
    ]
    results = pl.pallas_call(
        functools.partial(kernel, sizes),
        out_shape=tuple(pltpu.VMEM(shape, kind) for shape, kind in shapes),
        in_specs=[anywhere] * 5,
        out_specs=(vmem,) * 5,
        scratch_shapes=[
            pltpu.VMEM((1, blocks, width), f32),
            pltpu.VMEM((1, blocks), f32),
            pltpu.VMEM((3, owned, width), f32),
            pltpu.VMEM((part, width), f32),
            pltpu.VMEM((blocks, width), bf16),
            pltpu.VMEM((2 * n if mates else n, part, width), bf16),
            pltpu.VMEM((pair * fsdp, 3, owned, width), f32),
            pltpu.VMEM((3, part, width), f32),
            pltpu.VMEM((2 * pair * fsdp, owned, width), f32),
            pltpu.VMEM((owned, width), f32),
            pltpu.VMEM((lines, width), f32),
            pltpu.VMEM((n, lines, width), f32),
            pltpu.VMEM((lines, width), f32),
            pltpu.VMEM((lines, width), f32),
            pltpu.SemaphoreType.DMA((4,)),
            pltpu.SemaphoreType.DMA((2,)),
        ]
        + [pltpu.SemaphoreType.DMA] * 2
        + [pltpu.SemaphoreType.DMA((2,))]
        + [pltpu.SemaphoreType.DMA] * 6
        + (root_scratch if mates else [pltpu.SemaphoreType.DMA]),
        compiler_params=pltpu.CompilerParams(collective_id=0, has_side_effects=True),
    )(grads, last_peak.reshape(1, blocks), master, moment1, moment2)
    updated, first, second, weights, peak = pl.pallas_call(
        finish_kernel,
        out_shape=tuple(jax.ShapeDtypeStruct(shape, kind) for shape, kind in shapes),
        in_specs=[vmem] * 5,
        out_specs=(anywhere,) * 5,
        scratch_shapes=[pltpu.VMEM((3, owned, width), f32), pltpu.SemaphoreType.DMA((3,))],
    )(*(pltpu.with_memory_space_constraint(result, pltpu.VMEM) for result in results))
    return (updated, first, second, weights, peak.reshape(blocks))


def solution(mesh):
    sharded = P(AXES, None)
    return jax.shard_map(
        functools.partial(body, (mesh.shape["dp"], mesh.shape["fsdp"])),
        mesh=mesh,
        in_specs=(P(AXES, None, None), P(), sharded, sharded, sharded),
        out_specs=(sharded, sharded, sharded, P(), P()),
        check_vma=False,
    )
```
